32 devices in a mesh: dp: 4 (over y, z), sp: 8 (over x, core).
Axes of the slice: x: 4, y: 2, z: 2, core: 2. Of those that a mesh axis runs over, the one named last changes fastest.
The devices are a block of a 4x4x8 slice.
Arguments:
- x_in: bfloat16 [32, 512, 1024], P('dp', 'sp'), parts along dimension 0
- grad_y: bfloat16 [32, 512, 1024], P('dp', 'sp'), parts along dimension 0
- positions: int32 [2048], P(('dp', 'sp')), parts along dimension 0
- w_q: bfloat16 [1024, 2048], replicated
- w_k: bfloat16 [1024, 1024], replicated
- w_v: bfloat16 [1024, 1024], replicated
- w_o: bfloat16 [2048, 1024], replicated
- w_gate: bfloat16 [1024, 3072], replicated
- w_up: bfloat16 [1024, 3072], replicated
- w_down: bfloat16 [3072, 1024], replicated
- norm_gain: float32 [1024], replicated
- q_norm: float32 [16, 128], replicated
- k_norm: float32 [8, 128], replicated
Outputs:
- output 1: bfloat16 [32, 512, 1024], P('dp', 'sp'), parts along dimension 0
- output 2: bfloat16 [32, 512, 1024], P('dp', 'sp'), parts along dimension 0
- output 3: bfloat16 [4096, 2048], P('dp'), parts along dimension 0
- output 4: bfloat16 [4096, 1024], P('dp'), parts along dimension 0
- output 5: bfloat16 [4096, 1024], P('dp'), parts along dimension 0
- output 6: bfloat16 [8192, 1024], P('dp'), parts along dimension 0
- output 7: bfloat16 [4096, 3072], P('dp'), parts along dimension 0
- output 8: bfloat16 [4096, 3072], P('dp'), parts along dimension 0
- output 9: bfloat16 [12288, 1024], P('dp'), parts along dimension 0
- output 10: float32 [4096], P('dp'), parts along dimension 0
- output 11: float32 [64, 128], P('dp'), parts along dimension 0
- output 12: float32 [32, 128], P('dp'), parts along dimension 0
There are 4 independent parts. The reference program is written for one: setup_inputs(seed, part) draws one part's arguments, and reference() takes and returns one part's arrays. A program takes and returns all parts, laid end to end along the dimension named above; an argument that names none is the same for every part.
All inputs are finite; a program needn't handle non-finite values.
Results may differ from the reference program's by a relative error of at most 0.02.
Values are sent between devices in bfloat16 or wider.
A program may use at most 768 MiB of HBM per device.

```python
import jax
import jax.numpy as jnp
from jax import lax

BATCH_SIZE = 8
SEQ_LEN = 512
MODEL_DIM = 1024
FFN_DIM = 3072
NUM_HEADS = 16
NUM_KV = 8
HEAD_DIM = 128

NORM_EPS = 1e-5
ROPE_THETA = 75.0e6


def setup_inputs(seed: int = 0, part: int = 0) -> dict:
    root_key = jax.random.key(seed)
    part_keys = jax.random.split(jax.random.fold_in(root_key, part), 4)
    weight_keys = jax.random.split(root_key, 10)
    q_width = NUM_HEADS * HEAD_DIM
    kv_width = NUM_KV * HEAD_DIM
    act_shape = (BATCH_SIZE, SEQ_LEN, MODEL_DIM)
    pos_steps = jax.random.randint(part_keys[2], (SEQ_LEN,), 1, 3)
    offset = jax.random.randint(part_keys[3], (), 0, SEQ_LEN)

    def normal_weight(slot_index, num_rows, num_cols, fan_in):
        raw_draw = jax.random.normal(weight_keys[slot_index], (num_rows, num_cols), jnp.float32)
        return (raw_draw * fan_in ** -0.5).astype(jnp.bfloat16)

    return {
        'x_in': jax.random.normal(part_keys[0], act_shape, jnp.float32).astype(jnp.bfloat16),
        'grad_y': jax.random.normal(part_keys[1], act_shape, jnp.float32).astype(jnp.bfloat16),
        'positions': (offset + jnp.cumsum(pos_steps) - pos_steps[0]).astype(jnp.int32),
        'w_q': normal_weight(0, MODEL_DIM, q_width, MODEL_DIM),
        'w_k': normal_weight(1, MODEL_DIM, kv_width, MODEL_DIM),
        'w_v': normal_weight(2, MODEL_DIM, kv_width, MODEL_DIM),
        'w_o': normal_weight(3, q_width, MODEL_DIM, q_width),
        'w_gate': normal_weight(4, MODEL_DIM, FFN_DIM, MODEL_DIM),
        'w_up': normal_weight(5, MODEL_DIM, FFN_DIM, MODEL_DIM),
        'w_down': normal_weight(6, FFN_DIM, MODEL_DIM, FFN_DIM),
        'norm_gain': jax.random.uniform(weight_keys[7], (MODEL_DIM,), jnp.float32, 0.5, 1.5),
        'q_norm': jax.random.uniform(weight_keys[8], (NUM_HEADS, HEAD_DIM), jnp.float32, 0.5, 2.0),
        'k_norm': jax.random.uniform(weight_keys[9], (NUM_KV, HEAD_DIM), jnp.float32, 0.5, 2.0),
    }


def input_norm(x_f32, norm_gain):
    row_mean = jnp.mean(x_f32, axis=-1, keepdims=True)
    centered = x_f32 - row_mean
    row_var = jnp.mean(centered * centered, axis=-1, keepdims=True)
    return (centered * lax.rsqrt(row_var + NORM_EPS) * norm_gain).astype(jnp.bfloat16)


def rope_tables(positions):
    inv_freq = ROPE_THETA ** (-(jnp.arange(HEAD_DIM // 2, dtype=jnp.float32) * 2.0) / HEAD_DIM)
    angles = positions.astype(jnp.float32)[:, None] * inv_freq[None, :]
    return jnp.cos(angles), jnp.sin(angles)


def head_prepare(proj_in, norm_weight, cos_t, sin_t):
    proj_f32 = proj_in.astype(jnp.float32)
    row_mean = jnp.mean(proj_f32, axis=-1, keepdims=True)
    centered = proj_f32 - row_mean
    row_var = jnp.mean(centered * centered, axis=-1, keepdims=True)
    normed = centered * lax.rsqrt(row_var + NORM_EPS) * norm_weight
    pair_view = normed.reshape(normed.shape[:-1] + (normed.shape[-1] // 2, 2))
    even_part = pair_view[..., 0]
    odd_part = pair_view[..., 1]
    cos_rows = cos_t[:, None, :]
    sin_rows = sin_t[:, None, :]
    rotated = jnp.stack([even_part * cos_rows - odd_part * sin_rows, even_part * sin_rows + odd_part * cos_rows], axis=-1)
    return rotated.reshape(normed.shape).astype(jnp.bfloat16)


def head_attention(operands):
    q_head, k_head, v_head = operands
    scores = jnp.einsum('bqd,bsd->bqs', q_head.astype(jnp.float32), k_head.astype(jnp.float32)) * HEAD_DIM ** -0.5
    causal = jnp.arange(SEQ_LEN)[:, None] >= jnp.arange(SEQ_LEN)[None, :]
    attn_probs = jax.nn.softmax(jnp.where(causal, scores, -1e30), axis=-1).astype(jnp.bfloat16)
    attended = jnp.einsum('bqs,bsd->bqd', attn_probs.astype(jnp.float32), v_head.astype(jnp.float32))
    return attended.astype(jnp.bfloat16)


def layer_forward(x_in, positions, weights):
    w_q, w_k, w_v, w_o, w_gate, w_up, w_down, norm_gain, q_norm, k_norm = weights
    tokens = BATCH_SIZE * SEQ_LEN
    head_shape = (BATCH_SIZE, SEQ_LEN, NUM_HEADS, HEAD_DIM)
    kv_shape = (BATCH_SIZE, SEQ_LEN, NUM_KV, HEAD_DIM)
    x_f32 = x_in.astype(jnp.float32)
    normed = input_norm(x_f32, norm_gain).reshape(tokens, MODEL_DIM)
    q_proj = jnp.dot(normed, w_q, preferred_element_type=jnp.float32).astype(jnp.bfloat16).reshape(head_shape)
    k_proj = jnp.dot(normed, w_k, preferred_element_type=jnp.float32).astype(jnp.bfloat16).reshape(kv_shape)
    v_proj = jnp.dot(normed, w_v, preferred_element_type=jnp.float32).astype(jnp.bfloat16).reshape(kv_shape)
    cos_t, sin_t = rope_tables(positions)
    q_rot = head_prepare(q_proj, q_norm, cos_t, sin_t)
    k_rot = head_prepare(k_proj, k_norm, cos_t, sin_t)
    group_size = NUM_HEADS // NUM_KV
    q_major = jnp.moveaxis(q_rot, 2, 0)
    k_major = jnp.repeat(jnp.moveaxis(k_rot, 2, 0), group_size, axis=0)
    v_major = jnp.repeat(jnp.moveaxis(v_proj, 2, 0), group_size, axis=0)
    attended = lax.map(jax.checkpoint(head_attention), (q_major, k_major, v_major))
    attn_flat = jnp.moveaxis(attended, 0, 2).reshape(tokens, NUM_HEADS * HEAD_DIM)
    attn_out = jnp.dot(attn_flat, w_o, preferred_element_type=jnp.float32).astype(jnp.bfloat16)
    gate_pre = jnp.dot(normed, w_gate, preferred_element_type=jnp.float32)
    up_proj = jnp.dot(normed, w_up, preferred_element_type=jnp.float32)
    hidden = (jax.nn.silu(gate_pre) * up_proj).astype(jnp.bfloat16)
    mlp_out = jnp.dot(hidden, w_down, preferred_element_type=jnp.float32).astype(jnp.bfloat16)
    summed = x_f32 + attn_out.astype(jnp.float32).reshape(x_in.shape) + mlp_out.astype(jnp.float32).reshape(x_in.shape)
    return summed.astype(jnp.bfloat16)


def reference(x_in, grad_y, positions, w_q, w_k, w_v, w_o, w_gate, w_up, w_down, norm_gain, q_norm, k_norm):
    weights = (w_q, w_k, w_v, w_o, w_gate, w_up, w_down, norm_gain, q_norm, k_norm)
    y_out, layer_back = jax.vjp(lambda x_arg, w_arg: layer_forward(x_arg, positions, w_arg), x_in, weights)
    grad_x, weight_grads = layer_back(grad_y)
    return (y_out, grad_x, weight_grads[0], weight_grads[1], weight_grads[2], weight_grads[3], weight_grads[4], weight_grads[5], weight_grads[6], weight_grads[7], weight_grads[8], weight_grads[9])
```

```python
import functools

import jax
import jax.numpy as jnp
from jax import lax
from jax.experimental import pallas as pl
from jax.experimental.pallas import tpu as pltpu
from jax.sharding import PartitionSpec as P

NORM_EPS = 1e-5
ROPE_THETA = 75.0e6
F32 = jnp.float32
BF16 = jnp.bfloat16


def dot_nn(lhs, rhs):
    return lax.dot_general(lhs, rhs, (((1,), (0,)), ((), ())), preferred_element_type=F32)


def dot_nt(lhs, rhs):
    return lax.dot_general(lhs, rhs, (((1,), (1,)), ((), ())), preferred_element_type=F32)


def dot_tn(lhs, rhs):
    return lax.dot_general(lhs, rhs, (((0,), (0,)), ((), ())), preferred_element_type=F32)


def input_norm(x_f32, norm_gain):
    row_mean = jnp.mean(x_f32, axis=-1, keepdims=True)
    centered = x_f32 - row_mean
    row_var = jnp.mean(centered * centered, axis=-1, keepdims=True)
    return (centered * lax.rsqrt(row_var + NORM_EPS) * norm_gain).astype(BF16)


def swiglu(gate_pre, up_proj):
    return (jax.nn.silu(gate_pre) * up_proj).astype(BF16)


def swap_pairs(rows):
    width = rows.shape[1]
    lane = lax.broadcasted_iota(jnp.int32, rows.shape, 1)
    return jnp.where(lane % 2 == 0, pltpu.roll(rows, width - 1, 1), pltpu.roll(rows, 1, 1))


def head_forward(rows, weight, cos_t, sin_t):
    rows = rows.astype(F32)
    centered = rows - jnp.mean(rows, axis=-1, keepdims=True)
    scale = lax.rsqrt(jnp.mean(centered * centered, axis=-1, keepdims=True) + NORM_EPS)
    unit = centered * scale
    normed = unit * weight
    return (normed * cos_t + swap_pairs(normed) * sin_t).astype(BF16), unit, scale


def head_backward(grad, unit, scale, weight, cos_t, sin_t):
    grad = grad.astype(BF16).astype(F32)
    grad = grad * cos_t - swap_pairs(grad) * sin_t
    weight_grad = jnp.sum(grad * unit, axis=0, keepdims=True)
    grad = grad * weight
    along = jnp.mean(grad * unit, axis=-1, keepdims=True)
    grad = scale * (grad - jnp.mean(grad, axis=-1, keepdims=True) - unit * along)
    return grad.astype(BF16), weight_grad


def attention_kernel(qkv_ref, do_ref, cos_ref, sin_ref, qn_ref, kn_ref, o_ref, dqkv_ref, wn_ref, k_acc, v_acc, *, heads, dim, block):
    pieces, _, piece, _ = qkv_ref.shape
    full = pieces * piece
    cos_t, sin_t = cos_ref[...], sin_ref[...]
    score_scale = dim ** -0.5
    width = heads * dim

    def columns(ref, start, size):
        return ref[:, 0, :, start:start + size].reshape(full, size)

    def put(ref, start, rows):
        ref[:, 0, :, start:start + rows.shape[1]] = rows.reshape(pieces, piece, rows.shape[1])

    q_parts = [head_forward(columns(qkv_ref, h * dim, dim), qn_ref[h:h + 1, :], cos_t, sin_t) for h in range(heads)]
    k_rot, k_unit, k_scale = head_forward(columns(qkv_ref, width, dim), kn_ref[...], cos_t, sin_t)
    v_rows = columns(qkv_ref, width + dim, dim)
    do_parts = [columns(do_ref, h * dim, dim) for h in range(heads)]
    k_acc[...] = jnp.zeros_like(k_acc)
    v_acc[...] = jnp.zeros_like(v_acc)
    o_blocks, dq_blocks = [[] for _ in range(heads)], [[] for _ in range(heads)]
    for start in range(0, full, block):
        stop = start + block
        q_blk = jnp.concatenate([q_parts[h][0][start:stop] for h in range(heads)], axis=0)
        do_blk = jnp.concatenate([do_parts[h][start:stop] for h in range(heads)], axis=0)
        k_blk, v_blk = k_rot[:stop], v_rows[:stop]
        scores = dot_nt(q_blk, k_blk) * score_scale
        row = lax.broadcasted_iota(jnp.int32, scores.shape, 0) % block + start
        scores = jnp.where(row >= lax.broadcasted_iota(jnp.int32, scores.shape, 1), scores, -1e30)
        probs = jnp.exp(scores - jnp.max(scores, axis=-1, keepdims=True))
        probs = probs / jnp.sum(probs, axis=-1, keepdims=True)
        probs_b = probs.astype(BF16)
        o_blk = dot_nn(probs_b, v_blk).astype(BF16)
        d_probs = dot_nt(do_blk, v_blk)
        delta = jnp.sum(probs * d_probs, axis=-1, keepdims=True)
        d_scores = (probs * (d_probs - delta) * score_scale).astype(BF16)
        dq_blk = dot_nn(d_scores, k_blk)
        k_acc[0:stop, :] += dot_tn(d_scores, q_blk)
        v_acc[0:stop, :] += dot_tn(probs_b, do_blk)
        for h in range(heads):
            o_blocks[h].append(o_blk[h * block:(h + 1) * block])
            dq_blocks[h].append(dq_blk[h * block:(h + 1) * block])
    weight_grads = []
    for h in range(heads):
        put(o_ref, h * dim, jnp.concatenate(o_blocks[h], axis=0))
        _, unit, scale = q_parts[h]
        dq, weight_grad = head_backward(jnp.concatenate(dq_blocks[h], axis=0), unit, scale, qn_ref[h:h + 1, :], cos_t, sin_t)
        put(dqkv_ref, h * dim, dq)
        weight_grads.append(weight_grad)
    dk, weight_grad = head_backward(k_acc[...], k_unit, k_scale, kn_ref[...], cos_t, sin_t)
    put(dqkv_ref, width, dk)
    put(dqkv_ref, width + dim, v_acc[...].astype(BF16))
    weight_grads.append(weight_grad)

    @pl.when(pl.program_id(0) == 0)
    def _():
        wn_ref[...] = jnp.zeros_like(wn_ref)

    for i, weight_grad in enumerate(weight_grads):
        wn_ref[i:i + 1, :] += weight_grad


def attention(qkv, d_out, cos_t, sin_t, q_norm, k_norm):
    pieces, batch, piece, _ = qkv.shape
    heads, dim = q_norm.shape
    full = pieces * piece
    block = min(128, full)
    seq = lambda width: pl.BlockSpec((pieces, 1, piece, width), lambda b: (0, b, 0, 0))
    whole = lambda shape: pl.BlockSpec(shape, lambda b: (0,) * len(shape))
    return pl.pallas_call(
        functools.partial(attention_kernel, heads=heads, dim=dim, block=block),
        grid=(batch,),
        in_specs=[seq((heads + 2) * dim), seq(heads * dim), whole((full, dim)), whole((full, dim)), whole((heads, dim)), whole((1, dim))],
        out_specs=[seq(heads * dim), seq((heads + 2) * dim), whole((8, dim))],
        out_shape=[jax.ShapeDtypeStruct((pieces, batch, piece, heads * dim), BF16),
                   jax.ShapeDtypeStruct((pieces, batch, piece, (heads + 2) * dim), BF16),
                   jax.ShapeDtypeStruct((8, dim), F32)],
        scratch_shapes=[pltpu.VMEM((full, dim), F32), pltpu.VMEM((full, dim), F32)],
        cost_estimate=pl.CostEstimate(flops=14 * batch * heads * full * full * dim, bytes_accessed=batch * full * dim * 26, transcendentals=0),
    )(qkv, d_out, cos_t, sin_t, q_norm, k_norm)


def solution(mesh):
    n_sp = mesh.shape['sp']
    seq_spec = P('dp', 'sp', None)
    grad_spec = P('dp', None)

    def layer_step(x_in, grad_y, positions, w_q, w_k, w_v, w_o, w_gate, w_up, w_down, norm_gain, q_norm, k_norm):
        batch, piece, model = x_in.shape
        num_heads, dim = q_norm.shape
        num_kv = k_norm.shape[0]
        heads = num_heads // num_kv
        ffn = w_gate.shape[1]
        tokens = batch * piece
        me = lax.axis_index('sp')
        x_f32 = x_in.astype(F32)
        normed, norm_back = jax.vjp(input_norm, x_f32, norm_gain)
        dy_all = lax.all_gather(grad_y, 'sp', axis=0, tiled=False)
        n_all = lax.all_gather(normed, 'sp', axis=0, tiled=False)
        pos_all = lax.all_gather(positions, 'sp', axis=0, tiled=True)
        flat_norm = normed.reshape(tokens, model)
        flat_grad = grad_y.reshape(tokens, model)
        n_rows = n_all.reshape(n_sp * tokens, model)
        dy_rows = dy_all.reshape(n_sp * tokens, model)

        inv_freq = ROPE_THETA ** (-(jnp.arange(dim // 2, dtype=F32) * 2.0) / dim)
        angles = jnp.repeat(pos_all.astype(F32)[:, None] * inv_freq[None, :], 2, axis=1)
        sign = jnp.where(jnp.arange(dim) % 2 == 0, -1.0, 1.0).astype(F32)
        cos_t, sin_t = jnp.cos(angles), jnp.sin(angles) * sign[None, :]

        gate_pre = dot_nn(flat_norm, w_gate)
        up_proj = dot_nn(flat_norm, w_up)
        hidden, act_back = jax.vjp(swiglu, gate_pre, up_proj)
        mlp_out = dot_nn(hidden, w_down).astype(BF16)
        d_gate, d_up = act_back(dot_nt(flat_grad, w_down).astype(BF16))
        d_norm = dot_nt(d_gate.astype(BF16), w_gate) + dot_nt(d_up.astype(BF16), w_up)

        wq_mine = lax.dynamic_slice_in_dim(w_q, me * heads * dim, heads * dim, 1)
        wk_mine = lax.dynamic_slice_in_dim(w_k, me * dim, dim, 1)
        wv_mine = lax.dynamic_slice_in_dim(w_v, me * dim, dim, 1)
        wo_mine = lax.dynamic_slice_in_dim(w_o, me * heads * dim, heads * dim, 0)
        qkv = dot_nn(n_rows, jnp.concatenate([wq_mine, wk_mine, wv_mine], axis=1)).astype(BF16)
        d_attn = dot_nt(dy_rows, wo_mine).astype(BF16)
        qn_mine = lax.dynamic_slice_in_dim(q_norm, me * heads, heads, 0)
        kn_mine = lax.dynamic_slice_in_dim(k_norm, me, 1, 0)
        o_heads, dqkv, norm_grads = attention(qkv.reshape(n_sp, batch, piece, -1), d_attn.reshape(n_sp, batch, piece, -1), cos_t, sin_t, qn_mine, kn_mine)
        o_seq = lax.all_to_all(o_heads, 'sp', 0, 0, tiled=True)
        dqkv_seq = lax.all_to_all(dqkv, 'sp', 0, 0, tiled=True)
        dqkv_rows = dqkv.reshape(n_sp * tokens, -1)
        o_rows = o_heads.reshape(n_sp * tokens, -1)
        grad_qkv = dot_tn(n_rows, dqkv_rows).astype(BF16)
        grad_o = dot_tn(o_rows, dy_rows).astype(BF16)

        share = ffn // n_sp
        wg_mine = lax.dynamic_slice_in_dim(w_gate, me * share, share, 1)
        wu_mine = lax.dynamic_slice_in_dim(w_up, me * share, share, 1)
        wd_mine = lax.dynamic_slice_in_dim(w_down, me * share, share, 0)
        hid_cols, cols_back = jax.vjp(swiglu, dot_nn(n_rows, wg_mine), dot_nn(n_rows, wu_mine))
        dg_cols, du_cols = cols_back(dot_nt(dy_rows, wd_mine).astype(BF16))
        grad_gate = dot_tn(n_rows, dg_cols.astype(BF16)).astype(BF16)
        grad_up = dot_tn(n_rows, du_cols.astype(BF16)).astype(BF16)
        grad_down = dot_tn(hid_cols, dy_rows).astype(BF16)
        full_gate = lax.all_gather(grad_gate, 'sp', axis=1, tiled=True)
        full_up = lax.all_gather(grad_up, 'sp', axis=1, tiled=True)
        full_down = lax.all_gather(grad_down, 'sp', axis=0, tiled=True)
        full_o = lax.all_gather(grad_o, 'sp', axis=0, tiled=True)
        full_qkv = lax.all_gather(grad_qkv, 'sp', axis=0, tiled=False)
        unstack = lambda part: jnp.moveaxis(part, 0, 1).reshape(model, -1)
        full_q = unstack(full_qkv[:, :, :heads * dim])
        full_k = unstack(full_qkv[:, :, heads * dim:(heads + 1) * dim])
        full_v = unstack(full_qkv[:, :, (heads + 1) * dim:])

        o_seq = o_seq.reshape(n_sp, tokens, heads * dim)
        attn_out = lax.dot_general(o_seq, w_o.reshape(n_sp, heads * dim, model), (((0, 2), (0, 1)), ((), ())), preferred_element_type=F32).astype(BF16)
        y_out = (x_f32 + attn_out.astype(F32).reshape(x_in.shape) + mlp_out.astype(F32).reshape(x_in.shape)).astype(BF16)
        dqkv_seq = dqkv_seq.reshape(n_sp, tokens, -1)

        def back_rows(start, size, weight):
            return lax.dot_general(dqkv_seq[:, :, start:start + size], weight.reshape(model, n_sp, size), (((0, 2), (1, 2)), ((), ())), preferred_element_type=F32)

        d_norm = d_norm + back_rows(0, heads * dim, w_q) + back_rows(heads * dim, dim, w_k) + back_rows((heads + 1) * dim, dim, w_v)
        dx_norm, grad_gain = norm_back(d_norm.astype(BF16).reshape(x_in.shape))
        grad_x = (grad_y.astype(F32) + dx_norm).astype(BF16)

        small = jnp.concatenate([grad_gain.reshape(-1, dim), norm_grads[:heads + 1]], axis=0)
        small = lax.all_gather(small, 'sp', axis=0, tiled=False)
        gain_rows = model // dim
        full_gain = jnp.sum(small[:, :gain_rows], axis=0).reshape(model)
        full_qn = small[:, gain_rows:gain_rows + heads].reshape(num_heads, dim)
        full_kn = small[:, gain_rows + heads]
        return y_out, grad_x, full_q, full_k, full_v, full_o, full_gate, full_up, full_down, full_gain, full_qn, full_kn

    in_specs = (seq_spec, seq_spec, P(('dp', 'sp'))) + (P(),) * 10
    out_specs = (seq_spec, seq_spec) + (grad_spec,) * 7 + (P('dp'), grad_spec, grad_spec)
    return jax.shard_map(layer_step, mesh=mesh, in_specs=in_specs, out_specs=out_specs, check_vma=False)
```

```python
import functools

import jax
import jax.numpy as jnp
from jax import lax
from jax.experimental import pallas as pl
from jax.experimental.pallas import tpu as pltpu
from jax.sharding import PartitionSpec as P


NORM_EPS = 1e-5
ROPE_THETA = 75.0e6
F32 = jnp.float32
BF16 = jnp.bfloat16
MESH = pl.DeviceIdType.MESH


def dot_nn(lhs, rhs):
    return lax.dot_general(lhs, rhs, (((1,), (0,)), ((), ())), preferred_element_type=F32)


def dot_nt(lhs, rhs):
    return lax.dot_general(lhs, rhs, (((1,), (1,)), ((), ())), preferred_element_type=F32)


def swiglu_both(gate, up, d_hidden):
    sig = jax.nn.sigmoid(gate)
    act = gate * sig
    d_hidden = d_hidden.astype(BF16).astype(F32)
    d_gate = d_hidden * up * (sig * (1.0 + gate * (1.0 - sig)))
    return (act * up).astype(BF16), d_gate.astype(BF16), (d_hidden * act).astype(BF16)


def other_devices(count):
    me = lax.axis_index('sp')
    return [lax.rem(me + shift, count) for shift in range(1, count)]


def meet(count):
    barrier = pltpu.get_barrier_semaphore()
    for device in other_devices(count):
        pl.semaphore_signal(barrier, inc=1, device_id={'sp': device}, device_id_type=MESH)
    pl.semaphore_wait(barrier, count - 1)


def own_mlp_kernel(n_ref, dy_ref, wg_ref, wu_ref, wd_ref, rope_ref, m_ref, dn_ref, gn_ref, gdy_ref, rest_ref, grope_ref,
                   m_acc, send_sem, recv_sem, rope_send, rope_recv, local_sem, *, count):
    step = pl.program_id(0)
    last = pl.num_programs(0) - 1
    me = lax.axis_index('sp')
    right, left, across, partner = lax.rem(me + 2, count), lax.rem(me + count - 2, count), lax.rem(me + 4, count), me + 1 - 2 * lax.rem(me, 2)
    other = lambda device: device + 1 - 2 * lax.rem(device, 2)
    first = gn_ref.shape[1]
    rows = n_ref.shape[0]

    def send(index, src, into, slot, target):
        return pltpu.make_async_remote_copy(src_ref=src, dst_ref=into.at[slot], send_sem=send_sem.at[index], recv_sem=recv_sem.at[index],
                                            device_id={'sp': target}, device_id_type=MESH)

    def forward(index, ref, slot, target):
        return send(index, ref.at[slot], ref, slot, target)

    n_own, dy_own = n_ref.at[pl.ds(0, first)], dy_ref.at[pl.ds(0, first)]
    own_sends = lambda: [send(0, dy_own, gdy_ref, me, right), send(2, n_own, gn_ref, me, left), send(1, n_own, gn_ref, me, right),
                         send(3, dy_own, gdy_ref, me, left), send(4, n_own, gn_ref, me, partner), send(5, dy_own, gdy_ref, me, partner)]
    early = lambda: [forward(6, gdy_ref, left, right), forward(7, gn_ref, right, left), forward(8, gdy_ref, left, partner), forward(9, gn_ref, right, partner)]
    late = lambda: [forward(10, gn_ref, left, partner), forward(11, gdy_ref, right, partner), forward(12, gdy_ref, across, partner), forward(13, gn_ref, across, partner)]
    tables = lambda: [pltpu.make_async_remote_copy(src_ref=rope_ref, dst_ref=grope_ref.at[me], send_sem=rope_send.at[i], recv_sem=rope_recv.at[i],
                                                   device_id={'sp': device}, device_id_type=MESH) for i, device in enumerate(other_devices(count))]
    keep = lambda: [pltpu.make_async_copy(n_own, gn_ref.at[me], local_sem.at[0]), pltpu.make_async_copy(dy_own, gdy_ref.at[me], local_sem.at[1]),
                    pltpu.make_async_copy(n_ref.at[pl.ds(first, rows - first)], rest_ref.at[0], local_sem.at[2]),
                    pltpu.make_async_copy(dy_ref.at[pl.ds(first, rows - first)], rest_ref.at[1], local_sem.at[3]),
                    pltpu.make_async_copy(rope_ref, grope_ref.at[me], local_sem.at[4])]

    def arrived(index, ref, slot):
        send(index, ref.at[slot], ref, slot, partner).wait_recv()

    @pl.when(step == 0)
    def _():
        meet(count)
        for copy in own_sends() + tables() + keep():
            copy.start()

    @pl.when(step == last - 1)
    def _():
        arrived(0, gdy_ref, left)
        arrived(2, gn_ref, right)
        for copy in early():
            copy.start()

    n, dy = n_ref[...], dy_ref[...]
    wg, wu, wd = wg_ref[...], wu_ref[...], wd_ref[...]
    hidden, d_gate, d_up = swiglu_both(dot_nn(n, wg), dot_nn(n, wu), dot_nt(dy, wd))
    m_new = dot_nn(hidden, wd)
    dn_new = dot_nt(d_gate, wg) + dot_nt(d_up, wu)

    @pl.when(step == 0)
    def _():
        m_acc[...] = m_new
        dn_ref[...] = dn_new

    @pl.when(step > 0)
    def _():
        m_acc[...] += m_new
        dn_ref[...] += dn_new

    @pl.when(step == last)
    def _():
        m_ref[...] = m_acc[...].astype(BF16)
        late_copies = late()
        for copy, (index, ref, slot) in zip(late_copies, ((1, gn_ref, left), (3, gdy_ref, right), (6, gdy_ref, across), (7, gn_ref, across))):
            arrived(index, ref, slot)
            copy.start()
        for index, ref, slot in ((4, gn_ref, partner), (5, gdy_ref, partner), (8, gdy_ref, other(left)), (9, gn_ref, other(right)),
                                 (10, gn_ref, other(left)), (11, gdy_ref, other(right)), (12, gdy_ref, other(across)), (13, gn_ref, other(across))):
            arrived(index, ref, slot)
        for copy in own_sends() + early() + late_copies:
            copy.wait_send()
        for copy in tables():
            copy.wait()
        for copy in keep():
            copy.wait()


def own_mlp(n, dy, w_gate, w_up, w_down, rope, count, first, block):
    rows, model = n.shape
    ffn = w_gate.shape[1]
    whole = pl.BlockSpec((rows, model), lambda i: (0, 0))
    cols = pl.BlockSpec((model, block), lambda i: (0, i))
    away = pl.BlockSpec(memory_space=pl.ANY)
    dma = pltpu.SemaphoreType.DMA
    return pl.pallas_call(
        functools.partial(own_mlp_kernel, count=count),
        grid=(ffn // block,),
        in_specs=[whole, whole, cols, cols, pl.BlockSpec((block, model), lambda i: (i, 0)), pl.BlockSpec(rope.shape, lambda i: (0, 0, 0))],
        out_specs=[whole, whole, away, away, away, away],
        out_shape=[jax.ShapeDtypeStruct((rows, model), BF16), jax.ShapeDtypeStruct((rows, model), F32),
                   jax.ShapeDtypeStruct((count, first, model), BF16), jax.ShapeDtypeStruct((count, first, model), BF16),
                   jax.ShapeDtypeStruct((2, rows - first, model), BF16), jax.ShapeDtypeStruct((count,) + rope.shape, F32)],
        scratch_shapes=[pltpu.VMEM((rows, model), F32), dma((14,)), dma((14,)), dma((count - 1,)), dma((count - 1,)), dma((5,))],
        compiler_params=pltpu.CompilerParams(vmem_limit_bytes=50 * 2 ** 20, collective_id=0, has_side_effects=True),
        cost_estimate=pl.CostEstimate(flops=12 * rows * model * ffn, bytes_accessed=6 * model * ffn, transcendentals=0),
    )(n, dy, w_gate, w_up, w_down, rope)


def all_mlp_kernel(*refs, chunks, block, count):
    n_refs, dy_refs = refs[:chunks], refs[chunks:2 * chunks]
    (wg_ref, wu_ref, wd_ref, mix_ref, gg_ref, gu_ref, gd_ref, pg_ref, pu_ref, pd_ref, swap_ref,
     n_all, dy_all, n_t, dy_t, acc_g, acc_u, acc_d, swap_send, swap_recv, half_send, half_recv, own_sem) = refs[2 * chunks:]
    step = pl.program_id(0)
    last = pl.num_programs(0) - 1
    share = wg_ref.shape[1]
    me = lax.axis_index('sp')
    partner = me + 1 - 2 * lax.rem(me, 2)

    def swaps():
        return [pltpu.make_async_remote_copy(src_ref=mix_ref.at[device], dst_ref=swap_ref.at[me], send_sem=swap_send.at[i], recv_sem=swap_recv.at[i],
                                             device_id={'sp': device}, device_id_type=MESH) for i, device in enumerate(other_devices(count))]

    def halves(i):
        cols = pl.ds(i * block, block)
        return [pltpu.make_async_remote_copy(src_ref=src.at[index], dst_ref=dst.at[index], send_sem=half_send.at[i, j], recv_sem=half_recv.at[i, j],
                                             device_id={'sp': partner}, device_id_type=MESH)
                for j, (src, dst, index) in enumerate(((gg_ref, pg_ref, (slice(None), cols)), (gu_ref, pu_ref, (slice(None), cols)), (gd_ref, pd_ref, (cols,))))]

    keep = lambda: pltpu.make_async_copy(mix_ref.at[me], swap_ref.at[me], own_sem)

    @pl.when(step == 0)
    def _():
        meet(count)
        keep().start()
        for copy in swaps():
            copy.start()
        acc_g[...] = jnp.zeros_like(acc_g)
        acc_u[...] = jnp.zeros_like(acc_u)
        acc_d[...] = jnp.zeros_like(acc_d)

    start = 0
    for n_ref, dy_ref in zip(n_refs, dy_refs):
        size = n_ref.shape[-2]
        n_all[start:start + size, :] = n_ref[...].reshape(size, n_ref.shape[-1])
        dy_all[start:start + size, :] = dy_ref[...].reshape(size, n_ref.shape[-1])
        start += size
    n_t[...] = n_all[...].T
    dy_t[...] = dy_all[...].T

    @pl.loop(0, share // block)
    def _(i):
        cols = pl.ds(pl.multiple_of(i * block, block), block)
        n, dy = n_all[...], dy_all[...]
        hidden, d_gate, d_up = swiglu_both(dot_nn(n, wg_ref[:, cols]), dot_nn(n, wu_ref[:, cols]), dot_nt(dy, wd_ref[cols, :]))
        acc_g[:, cols] += dot_nn(n_t[...], d_gate)
        acc_u[:, cols] += dot_nn(n_t[...], d_up)
        acc_d[:, cols] += dot_nn(dy_t[...], hidden)

        @pl.when(step == last)
        def _():
            gg_ref[:, cols] = acc_g[:, cols].astype(BF16)
            gu_ref[:, cols] = acc_u[:, cols].astype(BF16)
            gd_ref[cols, :] = acc_d[:, cols].T.astype(BF16)

        for done in range(share // block - 1):
            @pl.when((step == last) & (i == done + 1))
            def _():
                for copy in halves(done):
                    copy.start()

    @pl.when(step == last)
    def _():
        for copy in swaps():
            copy.wait()
        keep().wait()
        for copy in halves(share // block - 1):
            copy.start()
        for i in range(share // block):
            for copy in halves(i):
                copy.wait()


def all_mlp(n_chunks, dy_chunks, w_gate, w_up, w_down, mix, block):
    count, _, model = n_chunks[0][0].shape[-3:]
    share = w_gate.shape[1] // 2

    def rows_of(part, which):
        if part.ndim == 3:
            return pl.BlockSpec((1,) + part.shape[1:], lambda i: (i, 0, 0))
        return pl.BlockSpec((1, 1) + part.shape[2:], lambda i: (i, which, 0, 0))

    chunks = n_chunks + dy_chunks
    tile = sum(part.shape[-2] for part, _ in n_chunks)
    one = pl.Buffered(1)
    core = lambda: lax.rem(lax.axis_index('sp'), 2)
    in_cols = pl.BlockSpec((model, share), lambda i: (0, core()), pipeline_mode=one)
    out_cols = pl.BlockSpec((model, share), lambda i: (0, 0), pipeline_mode=one)
    away = pl.BlockSpec(memory_space=pl.ANY)
    dma = pltpu.SemaphoreType.DMA
    grads = [jax.ShapeDtypeStruct((model, share), BF16), jax.ShapeDtypeStruct((model, share), BF16), jax.ShapeDtypeStruct((share, model), BF16)]
    return pl.pallas_call(
        functools.partial(all_mlp_kernel, chunks=len(n_chunks), block=block, count=count),
        grid=(count,),
        in_specs=[rows_of(*chunk) for chunk in chunks] + [in_cols, in_cols, pl.BlockSpec((share, model), lambda i: (core(), 0), pipeline_mode=one), away],
        out_specs=[out_cols, out_cols, pl.BlockSpec((share, model), lambda i: (0, 0), pipeline_mode=one)] + [away] * 4,
        out_shape=grads + grads + [jax.ShapeDtypeStruct(mix.shape, BF16)],
        scratch_shapes=[pltpu.VMEM((tile, model), BF16)] * 2 + [pltpu.VMEM((model, tile), BF16)] * 2 + [pltpu.VMEM((model, share), F32)] * 3
        + [dma((count - 1,)), dma((count - 1,)), dma((share // block, 3)), dma((share // block, 3)), dma],
        compiler_params=pltpu.CompilerParams(vmem_limit_bytes=61 * 2 ** 20, collective_id=1, has_side_effects=True),
        cost_estimate=pl.CostEstimate(flops=12 * count * tile * model * share, bytes_accessed=4 * model * count * tile + 12 * model * share, transcendentals=0),
    )(*[part for part, _ in chunks], w_gate, w_up, w_down, mix)


def swap_pairs(rows):
    width = rows.shape[1]
    lane = lax.broadcasted_iota(jnp.int32, rows.shape, 1)
    return jnp.where(lane % 2 == 0, pltpu.roll(rows, width - 1, 1), pltpu.roll(rows, 1, 1))


def head_forward(rows, weight, cos_t, sin_t):
    rows = rows.astype(F32)
    centered = rows - jnp.mean(rows, axis=-1, keepdims=True)
    scale = lax.rsqrt(jnp.mean(centered * centered, axis=-1, keepdims=True) + NORM_EPS)
    unit = centered * scale
    normed = unit * weight
    return (normed * cos_t + swap_pairs(normed) * sin_t).astype(BF16), unit, scale


def head_backward(grad, unit, scale, weight, cos_t, sin_t):
    grad = grad.astype(BF16).astype(F32)
    grad = grad * cos_t - swap_pairs(grad) * sin_t
    weight_grad = jnp.sum(grad * unit, axis=0, keepdims=True)
    grad = grad * weight
    along = jnp.mean(grad * unit, axis=-1, keepdims=True)
    grad = scale * (grad - jnp.mean(grad, axis=-1, keepdims=True) - unit * along)
    return grad.astype(BF16), weight_grad


def heads_kernel(me_ref, n_ref, dy_ref, wq_ref, wk_ref, wv_ref, wo_ref, cos_ref, sin_ref, qn_ref, kn_ref, *refs, heads, dim, block, first, last):
    sums, refs = ((), refs) if first else (refs[:3], refs[3:])
    mix_ref, wn_ref, *grad_refs, k_acc, v_acc, qkv_acc, o_acc = refs
    step = pl.program_id(0)
    pieces, piece, model = n_ref.shape[0], *n_ref.shape[-2:]
    full = pieces * piece
    cos_t, sin_t = cos_ref[...].reshape(full, dim), sin_ref[...].reshape(full, dim)
    score_scale = dim ** -0.5
    width = heads * dim

    def put(start, rows):
        mix_ref[:, 0, :, start:start + rows.shape[1]] = rows.reshape(pieces, piece, rows.shape[1])

    @pl.when(step == 0)
    def _():
        for into, given in zip((wn_ref, qkv_acc, o_acc), sums or (None,) * 3):
            into[...] = jnp.zeros_like(into) if given is None else given[...]

    n_rows = n_ref[...].reshape(full, model)
    dy_rows = dy_ref[...].reshape(full, model)
    q_proj = dot_nn(n_rows, wq_ref[...]).astype(BF16)
    k_proj = dot_nn(n_rows, wk_ref[...]).astype(BF16)
    v_rows = dot_nn(n_rows, wv_ref[...]).astype(BF16)
    d_out = dot_nt(dy_rows, wo_ref[...]).astype(BF16)
    q_weights = [qn_ref[pl.ds(me_ref[0] * heads + h, 1), :] for h in range(heads)]
    k_weight = kn_ref[pl.ds(me_ref[0], 1), :]
    q_parts = [head_forward(q_proj[:, h * dim:(h + 1) * dim], q_weights[h], cos_t, sin_t) for h in range(heads)]
    k_rot, k_unit, k_scale = head_forward(k_proj, k_weight, cos_t, sin_t)
    k_t, v_t = k_rot.T, v_rows.T
    o_blocks, dq_blocks = [[] for _ in range(heads)], [[] for _ in range(heads)]
    for start in range(full - block, -1, -block):
        stop = start + block
        q_blk = jnp.concatenate([q_parts[h][0][start:stop] for h in range(heads)], axis=0)
        do_blk = jnp.concatenate([d_out[start:stop, h * dim:(h + 1) * dim] for h in range(heads)], axis=0)
        k_blk, v_blk = k_rot[:stop], v_rows[:stop]
        scores = dot_nt(k_blk, q_blk)
        tail = scores[start:]
        key = lax.broadcasted_iota(jnp.int32, tail.shape, 0)
        query = lax.broadcasted_iota(jnp.int32, tail.shape, 1) % block
        tail = jnp.where(query >= key, tail, -1e30)
        scores = tail if start == 0 else jnp.concatenate([scores[:start], tail], axis=0)
        top = jnp.max(scores, axis=0, keepdims=True)
        probs = jnp.exp((scores - top) * score_scale)
        probs = probs * (1.0 / jnp.sum(probs, axis=0, keepdims=True))
        probs_b = probs.astype(BF16)
        o_blk = dot_nn(v_t[:, :stop], probs_b).astype(BF16)
        d_probs = dot_nt(v_blk, do_blk)
        delta = jnp.sum(probs * d_probs, axis=0, keepdims=True)
        d_scores = (probs * (d_probs - delta)).astype(BF16)
        dq_blk = dot_nn(k_t[:, :stop], d_scores) * score_scale
        dk_new, dv_new = dot_nn(d_scores, q_blk), dot_nn(probs_b, do_blk)
        if stop == full:
            k_acc[...], v_acc[...] = dk_new, dv_new
        else:
            k_acc[0:stop, :] += dk_new
            v_acc[0:stop, :] += dv_new
        for h in range(heads):
            o_blocks[h].append(o_blk[:, h * block:(h + 1) * block])
            dq_blocks[h].append(dq_blk[:, h * block:(h + 1) * block].T)
    for h in range(heads):
        o_t = jnp.concatenate(o_blocks[h][::-1], axis=1)
        put(h * dim, o_t.T)
        o_acc[h * dim:(h + 1) * dim, :] += dot_nn(o_t, dy_rows)
        _, unit, scale = q_parts[h]
        dq, weight_grad = head_backward(jnp.concatenate(dq_blocks[h][::-1], axis=0), unit, scale, q_weights[h], cos_t, sin_t)
        put(width + h * dim, dq)
        qkv_acc[h * dim:(h + 1) * dim, :] += dot_nn(dq.T, n_rows)
        wn_ref[h:h + 1, :] += weight_grad
    dk, weight_grad = head_backward(k_acc[...] * score_scale, k_unit, k_scale, k_weight, cos_t, sin_t)
    wn_ref[heads:heads + 1, :] += weight_grad
    dv = v_acc[...].astype(BF16)
    put(2 * width, dk)
    put(2 * width + dim, dv)
    qkv_acc[width:width + dim, :] += dot_nn(dk.T, n_rows)
    qkv_acc[width + dim:width + 2 * dim, :] += dot_nn(dv.T, n_rows)

    @pl.when(step == pl.num_programs(0) - 1)
    def _():
        if last:
            packed, = grad_refs
            qkv_size = qkv_acc.shape[0]
            size = o_acc.shape[0]
            packed[:, :qkv_size] = qkv_acc[...].T.astype(BF16)
            for i in range(model // size):
                packed[i * size:(i + 1) * size, qkv_size:] = o_acc[:, i * size:(i + 1) * size].astype(BF16)
        else:
            grad_refs[0][...] = qkv_acc[...]
            grad_refs[1][...] = o_acc[...]


def own_heads(me, n, dy, which, w_q, w_k, w_v, w_o, rope, q_norm, k_norm, sums, last):
    pieces, batch, piece, model = n.shape[0], *n.shape[-3:]
    num_heads, dim = q_norm.shape
    heads = num_heads // k_norm.shape[0]
    full = pieces * piece
    width = (heads + 2) * dim

    def seq(part, side):
        if part.ndim == 4:
            return pl.BlockSpec((pieces, 1, piece, model), lambda b, p: (0, b, 0, 0))
        return pl.BlockSpec((pieces, 1, 1, piece, model), lambda b, p: (0, side, b, 0, 0))

    whole = lambda shape: pl.BlockSpec(shape, lambda b, p: (0,) * len(shape))
    cols = lambda size: pl.BlockSpec((model, size), lambda b, p: (0, p[0]))
    table = lambda side: pl.BlockSpec((pieces, 1, piece, dim), lambda b, p: (0, side, 0, 0))
    mix_width = heads * dim + width
    if last:
        grads = [jax.ShapeDtypeStruct((model, mix_width), BF16)]
    else:
        grads = [jax.ShapeDtypeStruct((width, model), F32), jax.ShapeDtypeStruct((heads * dim, model), F32)]
    return pl.pallas_call(
        functools.partial(heads_kernel, heads=heads, dim=dim, block=min(128, full), first=not sums, last=last),
        grid_spec=pltpu.PrefetchScalarGridSpec(
            num_scalar_prefetch=1,
            grid=(batch,),
            in_specs=[seq(n, which[0]), seq(dy, which[1]), cols(heads * dim), cols(dim), cols(dim), pl.BlockSpec((heads * dim, model), lambda b, p: (p[0], 0)),
                      table(0), table(1), whole(q_norm.shape), whole(k_norm.shape)] + [whole(part.shape) for part in sums],
            out_specs=[pl.BlockSpec((pieces, 1, piece, mix_width), lambda b, p: (0, b, 0, 0)), whole((8, dim))] + [whole(part.shape) for part in grads],
            scratch_shapes=[pltpu.VMEM((full, dim), F32), pltpu.VMEM((full, dim), F32), pltpu.VMEM((width, model), F32), pltpu.VMEM((heads * dim, model), F32)],
        ),
        out_shape=[jax.ShapeDtypeStruct((pieces, batch, piece, mix_width), BF16), jax.ShapeDtypeStruct((8, dim), F32)] + grads,
        compiler_params=pltpu.CompilerParams(vmem_limit_bytes=56 * 2 ** 20),
        cost_estimate=pl.CostEstimate(flops=batch * full * (14 * heads * full * dim + 4 * model * (width + heads * dim)),
                                      bytes_accessed=4 * batch * full * model, transcendentals=0),
    )(me, n, dy, w_q, w_k, w_v, w_o, rope, rope, q_norm, k_norm, *sums)


def norm_kernel(x_ref, gain_ref, n_ref):
    x = x_ref[...].astype(F32)
    centered = x - jnp.mean(x, axis=-1, keepdims=True)
    scale = lax.rsqrt(jnp.mean(centered * centered, axis=-1, keepdims=True) + NORM_EPS)
    n_ref[...] = (centered * scale * gain_ref[...]).astype(BF16)


def input_norm(x, gain):
    rows, model = x.shape
    tile = rows // 4
    return pl.pallas_call(
        norm_kernel,
        grid=(rows // tile,),
        in_specs=[pl.BlockSpec((tile, model), lambda i: (i, 0)), pl.BlockSpec((1, model), lambda i: (0, 0))],
        out_specs=pl.BlockSpec((tile, model), lambda i: (i, 0)),
        out_shape=jax.ShapeDtypeStruct((rows, model), BF16),
        cost_estimate=pl.CostEstimate(flops=8 * rows * model, bytes_accessed=4 * rows * model, transcendentals=0),
    )(x, gain)


def finish_kernel(core_ref, *refs, chunks, parts):
    mix_refs = refs[:chunks]
    (x_ref, dy_ref, m_ref, dn_ref, gain_ref, wq_ref, wk_ref, wv_ref, wo_ref, packed_ref, gg_ref, gu_ref, gd_ref, pg_ref, pu_ref, pd_ref,
     y_ref, dx_ref, gain_grad_ref, fq_ref, fk_ref, fv_ref, fo_ref, fg_ref, fu_ref, fd_ref,
     mix, a_acc, d_acc, packed_buf, col_buf, row_buf, in_sem, out_sem) = refs[chunks:]
    step = pl.program_id(0)
    steps = pl.num_programs(0)
    o_size, k_size = parts
    share = gg_ref.shape[1]
    col_rows, row_rows = col_buf.shape[2], row_buf.shape[2]
    core = core_ref[0]

    def fetches(at):
        slot = lax.rem(at, 2)
        cols = pl.ds(pl.multiple_of(at * col_rows, col_rows), col_rows)
        rows = pl.ds(pl.multiple_of(at * row_rows, row_rows), row_rows)
        pairs = [(packed_ref.at[at], packed_buf.at[slot])]
        pairs += [(ref.at[cols], col_buf.at[slot, i]) for i, ref in enumerate((gg_ref, gu_ref, pg_ref, pu_ref))]
        pairs += [(ref.at[rows], row_buf.at[slot, i]) for i, ref in enumerate((gd_ref, pd_ref))]
        return [pltpu.make_async_copy(src, dst, in_sem.at[slot, i]) for i, (src, dst) in enumerate(pairs)]

    def places(at):
        slot = lax.rem(at, 2)
        buf = packed_buf.at[slot]
        model = buf.shape[0]
        at_o, at_k = pl.ds(pl.multiple_of(at * o_size, o_size), o_size), pl.ds(pl.multiple_of(at * k_size, k_size), k_size)
        pairs = [(buf.at[:, pl.ds(0, o_size)], fq_ref.at[:, at_o]), (buf.at[:, pl.ds(o_size, k_size)], fk_ref.at[:, at_k]),
                 (buf.at[:, pl.ds(o_size + k_size, k_size)], fv_ref.at[:, at_k])]
        pairs += [(buf.at[pl.ds(i * o_size, o_size), pl.ds(o_size + 2 * k_size, o_size)], fo_ref.at[at_o, pl.ds(i * o_size, o_size)]) for i in range(model // o_size)]
        cols = pl.ds(pl.multiple_of(at * col_rows, col_rows), col_rows)
        mine, theirs = pl.multiple_of(core * share, share), pl.multiple_of((1 - core) * share, share)
        pairs += [(col_buf.at[slot, i], ref.at[cols, pl.ds(start, share)]) for i, (ref, start) in enumerate(((fg_ref, mine), (fu_ref, mine), (fg_ref, theirs), (fu_ref, theirs)))]
        pairs += [(row_buf.at[slot, i], fd_ref.at[pl.ds(pl.multiple_of(start + at * row_rows, row_rows), row_rows)]) for i, start in enumerate((mine, theirs))]
        return [pltpu.make_async_copy(src, dst, out_sem.at[slot, i]) for i, (src, dst) in enumerate(pairs)]

    @pl.when(step == 0)
    def _():
        for copy in fetches(0):
            copy.start()

    start = 0
    for ref in mix_refs:
        mix[start:start + ref.shape[1], :] = ref[0]
        start += ref.shape[1]
    a_new = dot_nn(mix[:, :o_size], wo_ref[...])
    d_new = dot_nt(mix[:, o_size:2 * o_size], wq_ref[...])
    d_new += dot_nt(mix[:, 2 * o_size:2 * o_size + k_size], wk_ref[...]) + dot_nt(mix[:, 2 * o_size + k_size:], wv_ref[...])

    @pl.when(step == 0)
    def _():
        a_acc[...] = a_new
        d_acc[...] = d_new + dn_ref[...]

    @pl.when(step > 0)
    def _():
        a_acc[...] += a_new
        d_acc[...] += d_new

    for copy in fetches(step):
        copy.wait()
    for copy in places(step):
        copy.start()

    @pl.when(step > 0)
    def _():
        for copy in places(step - 1):
            copy.wait()

    @pl.when(step < steps - 1)
    def _():
        for copy in fetches(step + 1):
            copy.start()

    @pl.when(step == steps - 1)
    def _():
        x = x_ref[...].astype(F32)
        y_ref[...] = (x + a_acc[...].astype(BF16).astype(F32) + m_ref[...].astype(F32)).astype(BF16)
        centered = x - jnp.mean(x, axis=-1, keepdims=True)
        scale = lax.rsqrt(jnp.mean(centered * centered, axis=-1, keepdims=True) + NORM_EPS)
        unit = centered * scale
        grad = d_acc[...].astype(BF16).astype(F32)
        gain_grad_ref[...] = jnp.sum(grad * unit, axis=0, keepdims=True)
        grad = grad * gain_ref[...]
        along = jnp.mean(grad * unit, axis=-1, keepdims=True)
        grad = scale * (grad - jnp.mean(grad, axis=-1, keepdims=True) - unit * along)
        dx_ref[...] = (dy_ref[...].astype(F32) + grad).astype(BF16)
        for copy in places(step):
            copy.wait()


def finish(core, mixes, x, dy, mlp_out, d_norm, gain, w_q, w_k, w_v, w_o, packed, own_grads, partner_grads, o_size, k_size):
    rows, model = x.shape
    pieces, _, width = mixes[0].shape
    share = own_grads[0].shape[1]
    whole = pl.BlockSpec((rows, model), lambda i, c: (0, 0))
    row = pl.BlockSpec((1, model), lambda i, c: (0, 0))
    cols = lambda size: pl.BlockSpec((model, size), lambda i, c: (0, i))
    away = pl.BlockSpec(memory_space=pl.ANY)
    bf16 = lambda *shape: jax.ShapeDtypeStruct(shape, BF16)
    return pl.pallas_call(
        functools.partial(finish_kernel, chunks=len(mixes), parts=(o_size, k_size)),
        grid_spec=pltpu.PrefetchScalarGridSpec(
            num_scalar_prefetch=1,
            grid=(pieces,),
            in_specs=[pl.BlockSpec((1, mix.shape[1], width), lambda i, c: (i, 0, 0)) for mix in mixes] + [whole] * 4
            + [row, cols(o_size), cols(k_size), cols(k_size), pl.BlockSpec((o_size, model), lambda i, c: (i, 0))] + [away] * 7,
            out_specs=[whole, whole, row] + [away] * 7,
            scratch_shapes=[pltpu.VMEM((rows, width), BF16), pltpu.VMEM((rows, model), F32), pltpu.VMEM((rows, model), F32),
                            pltpu.VMEM((2,) + packed.shape[1:], BF16), pltpu.VMEM((2, 4, model // pieces, share), BF16), pltpu.VMEM((2, 2, share // pieces, model), BF16),
                            pltpu.SemaphoreType.DMA((2, 7)), pltpu.SemaphoreType.DMA((2, 9 + model // o_size))],
        ),
        out_shape=[bf16(rows, model), bf16(rows, model), jax.ShapeDtypeStruct((1, model), F32)]
        + [bf16(*weight.shape) for weight in (w_q, w_k, w_v, w_o)] + [bf16(model, 2 * share), bf16(model, 2 * share), bf16(2 * share, model)],
        compiler_params=pltpu.CompilerParams(vmem_limit_bytes=56 * 2 ** 20),
        cost_estimate=pl.CostEstimate(flops=2 * pieces * rows * width * model, bytes_accessed=14 * rows * model + 2 * pieces * width * (rows + model), transcendentals=0),
    )(core, *mixes, x, dy, mlp_out, d_norm, gain, w_q, w_k, w_v, w_o, packed, *own_grads, *partner_grads)


def share_kernel(part_ref, all_ref, send_sem, recv_sem, *, count):
    me = lax.axis_index('sp')
    meet(count)
    all_ref[pl.ds(me, 1)] = part_ref[...][None]
    copies = [pltpu.make_async_remote_copy(src_ref=part_ref, dst_ref=all_ref.at[me], send_sem=send_sem.at[i], recv_sem=recv_sem.at[i],
                                           device_id={'sp': device}, device_id_type=MESH) for i, device in enumerate(other_devices(count))]
    for copy in copies:
        copy.start()
    for copy in copies:
        copy.wait()


def share_small(part, count):
    vmem = pl.BlockSpec(memory_space=pltpu.VMEM)
    return pl.pallas_call(
        functools.partial(share_kernel, count=count),
        in_specs=[vmem],
        out_specs=vmem,
        out_shape=jax.ShapeDtypeStruct((count,) + part.shape, part.dtype),
        scratch_shapes=[pltpu.SemaphoreType.DMA((count - 1,)), pltpu.SemaphoreType.DMA((count - 1,))],
        compiler_params=pltpu.CompilerParams(collective_id=2, has_side_effects=True),
    )(part)


def solution(mesh):
    n_sp = mesh.shape['sp']
    seq_spec = P('dp', 'sp', None)
    grad_spec = P('dp', None)

    def layer_step(x_in, grad_y, positions, w_q, w_k, w_v, w_o, w_gate, w_up, w_down, norm_gain, q_norm, k_norm):
        batch, piece, model = x_in.shape
        num_heads, dim = q_norm.shape
        heads = num_heads // k_norm.shape[0]
        ffn = w_gate.shape[1]
        tokens = batch * piece
        me = lax.axis_index('sp')
        me_arr = me.reshape(1)
        split = (batch * 5) // 8
        gain_row = norm_gain.reshape(1, model)
        x_rows, dy_own = x_in.reshape(tokens, model), grad_y.reshape(tokens, model)
        n_own = input_norm(x_rows, gain_row)

        inv_freq = ROPE_THETA ** (-(jnp.arange(dim // 2, dtype=F32) * 2.0) / dim)
        angles = jnp.repeat(positions.astype(F32)[:, None] * inv_freq[None, :], 2, axis=1)
        sign = jnp.where(jnp.arange(dim) % 2 == 0, -1.0, 1.0).astype(F32)
        rope_own = jnp.stack([jnp.cos(angles), jnp.sin(angles) * sign[None, :]])

        mlp_out, d_norm, n_0, dy_0, rest, rope = own_mlp(n_own, dy_own, w_gate, w_up, w_down, rope_own, n_sp, split * piece, min(512, ffn))
        rest = lax.all_gather(rest, 'sp', axis=0, tiled=False)

        by_seq = lambda part: part.reshape(part.shape[:-2] + (-1, piece, part.shape[-1]))
        mix_0, *sums = own_heads(me_arr, by_seq(n_0), by_seq(dy_0), (0, 0), w_q, w_k, w_v, w_o, rope, q_norm, k_norm, (), False)
        mix_0 = lax.all_to_all(mix_0, 'sp', 0, 0, tiled=True)
        mix_1, norm_grads, packed = own_heads(me_arr, by_seq(rest), by_seq(rest), (0, 1), w_q, w_k, w_v, w_o, rope, q_norm, k_norm, tuple(sums), True)
        packed_all = lax.all_gather(packed, 'sp', axis=0, tiled=False)

        rows = lambda part: part.reshape(n_sp, -1, part.shape[-1])
        *grads, mix_1 = all_mlp([(n_0, 0), (rest, 0)], [(dy_0, 0), (rest, 1)], w_gate, w_up, w_down, rows(mix_1), ffn // 6)

        y_out, grad_x, grad_gain, *full = finish((me % 2).reshape(1), (rows(mix_0), mix_1), x_rows, dy_own, mlp_out, d_norm, gain_row, w_q, w_k, w_v, w_o,
                                                 packed_all, grads[:3], grads[3:], heads * dim, dim)

        gain_rows = model // dim
        small = jnp.concatenate([grad_gain.reshape(gain_rows, dim), norm_grads], axis=0)
        small = share_small(small, n_sp)
        full_gain = jnp.sum(small[:, :gain_rows], axis=0).reshape(model)
        full_qn = small[:, gain_rows:gain_rows + heads].reshape(num_heads, dim)
        full_kn = small[:, gain_rows + heads]
        return (y_out.reshape(x_in.shape), grad_x.reshape(x_in.shape), *full, full_gain, full_qn, full_kn)

    in_specs = (seq_spec, seq_spec, P(('dp', 'sp'))) + (P(),) * 10
    out_specs = (seq_spec, seq_spec) + (grad_spec,) * 7 + (P('dp'), grad_spec, grad_spec)
    return jax.shard_map(layer_step, mesh=mesh, in_specs=in_specs, out_specs=out_specs, check_vma=False)
```

```python
import functools

import jax
import jax.numpy as jnp
from jax import lax
from jax.experimental import pallas as pl
from jax.experimental.pallas import tpu as pltpu
from jax.sharding import PartitionSpec as P

NORM_EPS = 1e-5
ROPE_THETA = 75.0e6
F32 = jnp.float32
BF16 = jnp.bfloat16
MESH = pl.DeviceIdType.MESH


def dot_nn(lhs, rhs):
    return lax.dot_general(lhs, rhs, (((1,), (0,)), ((), ())), preferred_element_type=F32)


def dot_nt(lhs, rhs):
    return lax.dot_general(lhs, rhs, (((1,), (1,)), ((), ())), preferred_element_type=F32)


def swiglu_both(gate, up, d_hidden):
    sig = jax.nn.sigmoid(gate)
    act = gate * sig
    d_hidden = d_hidden.astype(BF16).astype(F32)
    d_gate = d_hidden * up * (sig * (1.0 + gate * (1.0 - sig)))
    return (act * up).astype(BF16), d_gate.astype(BF16), (d_hidden * act).astype(BF16)


def other_devices(count):
    me = lax.axis_index('sp')
    return [lax.rem(me + shift, count) for shift in range(1, count)]


def meet(count):
    barrier = pltpu.get_barrier_semaphore()
    for device in other_devices(count):
        pl.semaphore_signal(barrier, inc=1, device_id={'sp': device}, device_id_type=MESH)
    pl.semaphore_wait(barrier, count - 1)


def all_mlp_kernel(*refs, chunks, block, count):
    n_refs, dy_refs = refs[:chunks], refs[chunks:2 * chunks]
    (wg_ref, wu_ref, wd_ref, mix_ref, gg_ref, gu_ref, gd_ref, pg_ref, pu_ref, pd_ref, swap_ref,
     n_all, dy_all, n_t, dy_t, acc_g, acc_u, acc_d, swap_send, swap_recv, half_send, half_recv, own_sem) = refs[2 * chunks:]
    step = pl.program_id(0)
    last = pl.num_programs(0) - 1
    share = wg_ref.shape[1]
    me = lax.axis_index('sp')
    partner = me + 1 - 2 * lax.rem(me, 2)

    def swaps():
        return [pltpu.make_async_remote_copy(src_ref=mix_ref.at[device], dst_ref=swap_ref.at[me], send_sem=swap_send.at[i], recv_sem=swap_recv.at[i],
                                             device_id={'sp': device}, device_id_type=MESH) for i, device in enumerate(other_devices(count))]

    def halves(i):
        cols = pl.ds(i * block, block)
        return [pltpu.make_async_remote_copy(src_ref=src.at[index], dst_ref=dst.at[index], send_sem=half_send.at[i, j], recv_sem=half_recv.at[i, j],
                                             device_id={'sp': partner}, device_id_type=MESH)
                for j, (src, dst, index) in enumerate(((gg_ref, pg_ref, (slice(None), cols)), (gu_ref, pu_ref, (slice(None), cols)), (gd_ref, pd_ref, (cols,))))]

    keep = lambda: pltpu.make_async_copy(mix_ref.at[me], swap_ref.at[me], own_sem)

    @pl.when(step == 0)
    def _():
        meet(count)
        keep().start()
        for copy in swaps():
            copy.start()
        acc_g[...] = jnp.zeros_like(acc_g)
        acc_u[...] = jnp.zeros_like(acc_u)
        acc_d[...] = jnp.zeros_like(acc_d)

    start = 0
    for n_ref, dy_ref in zip(n_refs, dy_refs):
        size = n_ref.shape[-2]
        n_all[start:start + size, :] = n_ref[...].reshape(size, n_ref.shape[-1])
        dy_all[start:start + size, :] = dy_ref[...].reshape(size, n_ref.shape[-1])
        start += size
    n_t[...] = n_all[...].T
    dy_t[...] = dy_all[...].T

    @pl.loop(0, share // block)
    def _(i):
        cols = pl.ds(pl.multiple_of(i * block, block), block)
        n, dy = n_all[...], dy_all[...]
        hidden, d_gate, d_up = swiglu_both(dot_nn(n, wg_ref[:, cols]), dot_nn(n, wu_ref[:, cols]), dot_nt(dy, wd_ref[cols, :]))
        acc_g[:, cols] += dot_nn(n_t[...], d_gate)
        acc_u[:, cols] += dot_nn(n_t[...], d_up)
        acc_d[:, cols] += dot_nn(dy_t[...], hidden)

        @pl.when(step == last)
        def _():
            gg_ref[:, cols] = acc_g[:, cols].astype(BF16)
            gu_ref[:, cols] = acc_u[:, cols].astype(BF16)
            gd_ref[cols, :] = acc_d[:, cols].T.astype(BF16)

        for done in range(share // block - 1):
            @pl.when((step == last) & (i == done + 1))
            def _():
                for copy in halves(done):
                    copy.start()

    @pl.when(step == last)
    def _():
        for copy in swaps():
            copy.wait()
        keep().wait()
        for copy in halves(share // block - 1):
            copy.start()
        for i in range(share // block):
            for copy in halves(i):
                copy.wait()


def all_mlp(n_chunks, dy_chunks, w_gate, w_up, w_down, mix, block):
    count, _, model = n_chunks[0][0].shape[-3:]
    share = w_gate.shape[1] // 2

    def rows_of(part, which):
        if part.ndim == 3:
            return pl.BlockSpec((1,) + part.shape[1:], lambda i: (i, 0, 0))
        return pl.BlockSpec((1, 1) + part.shape[2:], lambda i: (i, which, 0, 0))

    chunks = n_chunks + dy_chunks
    tile = sum(part.shape[-2] for part, _ in n_chunks)
    one = pl.Buffered(1)
    core = lambda: lax.rem(lax.axis_index('sp'), 2)
    in_cols = pl.BlockSpec((model, share), lambda i: (0, core()), pipeline_mode=one)
    out_cols = pl.BlockSpec((model, share), lambda i: (0, 0), pipeline_mode=one)
    away = pl.BlockSpec(memory_space=pl.ANY)
    dma = pltpu.SemaphoreType.DMA
    grads = [jax.ShapeDtypeStruct((model, share), BF16), jax.ShapeDtypeStruct((model, share), BF16), jax.ShapeDtypeStruct((share, model), BF16)]
    return pl.pallas_call(
        functools.partial(all_mlp_kernel, chunks=len(n_chunks), block=block, count=count),
        grid=(count,),
        in_specs=[rows_of(*chunk) for chunk in chunks] + [in_cols, in_cols, pl.BlockSpec((share, model), lambda i: (core(), 0), pipeline_mode=one), away],
        out_specs=[out_cols, out_cols, pl.BlockSpec((share, model), lambda i: (0, 0), pipeline_mode=one)] + [away] * 4,
        out_shape=grads + grads + [jax.ShapeDtypeStruct(mix.shape, BF16)],
        scratch_shapes=[pltpu.VMEM((tile, model), BF16)] * 2 + [pltpu.VMEM((model, tile), BF16)] * 2 + [pltpu.VMEM((model, share), F32)] * 3
        + [dma((count - 1,)), dma((count - 1,)), dma((share // block, 3)), dma((share // block, 3)), dma],
        compiler_params=pltpu.CompilerParams(vmem_limit_bytes=61 * 2 ** 20, collective_id=1, has_side_effects=True),
        cost_estimate=pl.CostEstimate(flops=12 * count * tile * model * share, bytes_accessed=4 * model * count * tile + 12 * model * share, transcendentals=0),
    )(*[part for part, _ in chunks], w_gate, w_up, w_down, mix)


def swap_pairs(rows):
    width = rows.shape[1]
    lane = lax.broadcasted_iota(jnp.int32, rows.shape, 1)
    return jnp.where(lane % 2 == 0, pltpu.roll(rows, width - 1, 1), pltpu.roll(rows, 1, 1))


def head_forward(rows, weight, cos_t, sin_t):
    rows = rows.astype(F32)
    centered = rows - jnp.mean(rows, axis=-1, keepdims=True)
    scale = lax.rsqrt(jnp.mean(centered * centered, axis=-1, keepdims=True) + NORM_EPS)
    unit = centered * scale
    normed = unit * weight
    return (normed * cos_t + swap_pairs(normed) * sin_t).astype(BF16), unit, scale


def head_backward(grad, unit, scale, weight, cos_t, sin_t):
    grad = grad.astype(BF16).astype(F32)
    grad = grad * cos_t - swap_pairs(grad) * sin_t
    weight_grad = jnp.sum(grad * unit, axis=0, keepdims=True)
    grad = grad * weight
    along = jnp.mean(grad * unit, axis=-1, keepdims=True)
    grad = scale * (grad - jnp.mean(grad, axis=-1, keepdims=True) - unit * along)
    return grad.astype(BF16), weight_grad


def one_sequence(me, n_rows, dy_rows, cos_t, sin_t, wq_ref, wk_ref, wv_ref, wo_ref, qn_ref, kn_ref, mix_ref, wn_ref, k_acc, v_acc, qkv_acc, o_acc, heads, dim, block):
    pieces, _, piece, _ = mix_ref.shape
    full = pieces * piece
    score_scale = dim ** -0.5
    width = heads * dim

    def put(start, rows):
        mix_ref[:, 0, :, start:start + rows.shape[1]] = rows.reshape(pieces, piece, rows.shape[1])

    q_proj = dot_nn(n_rows, wq_ref[...]).astype(BF16)
    k_proj = dot_nn(n_rows, wk_ref[...]).astype(BF16)
    v_rows = dot_nn(n_rows, wv_ref[...]).astype(BF16)
    d_out = dot_nt(dy_rows, wo_ref[...]).astype(BF16)
    q_weights = [qn_ref[pl.ds(me * heads + h, 1), :] for h in range(heads)]
    k_weight = kn_ref[pl.ds(me, 1), :]
    q_parts = [head_forward(q_proj[:, h * dim:(h + 1) * dim], q_weights[h], cos_t, sin_t) for h in range(heads)]
    k_rot, k_unit, k_scale = head_forward(k_proj, k_weight, cos_t, sin_t)
    k_t, v_t = k_rot.T, v_rows.T
    o_blocks, dq_blocks = [[] for _ in range(heads)], [[] for _ in range(heads)]
    for start in range(full - block, -1, -block):
        stop = start + block
        q_blk = jnp.concatenate([q_parts[h][0][start:stop] for h in range(heads)], axis=0)
        do_blk = jnp.concatenate([d_out[start:stop, h * dim:(h + 1) * dim] for h in range(heads)], axis=0)
        k_blk, v_blk = k_rot[:stop], v_rows[:stop]
        scores = dot_nt(k_blk, q_blk)
        tail = scores[start:]
        key = lax.broadcasted_iota(jnp.int32, tail.shape, 0)
        query = lax.broadcasted_iota(jnp.int32, tail.shape, 1) % block
        tail = jnp.where(query >= key, tail, -1e30)
        scores = tail if start == 0 else jnp.concatenate([scores[:start], tail], axis=0)
        top = jnp.max(scores, axis=0, keepdims=True)
        probs = jnp.exp((scores - top) * score_scale)
        probs = probs * (1.0 / jnp.sum(probs, axis=0, keepdims=True))
        probs_b = probs.astype(BF16)
        o_blk = dot_nn(v_t[:, :stop], probs_b).astype(BF16)
        d_probs = dot_nt(v_blk, do_blk)
        delta = jnp.sum(probs * d_probs, axis=0, keepdims=True)
        d_scores = (probs * (d_probs - delta)).astype(BF16)
        dq_blk = dot_nn(k_t[:, :stop], d_scores) * score_scale
        dk_new, dv_new = dot_nn(d_scores, q_blk), dot_nn(probs_b, do_blk)
        if stop == full:
            k_acc[...], v_acc[...] = dk_new, dv_new
        else:
            k_acc[0:stop, :] += dk_new
            v_acc[0:stop, :] += dv_new
        for h in range(heads):
            o_blocks[h].append(o_blk[:, h * block:(h + 1) * block])
            dq_blocks[h].append(dq_blk[:, h * block:(h + 1) * block].T)
    for h in range(heads):
        o_t = jnp.concatenate(o_blocks[h][::-1], axis=1)
        put(h * dim, o_t.T)
        o_acc[h * dim:(h + 1) * dim, :] += dot_nn(o_t, dy_rows)
        _, unit, scale = q_parts[h]
        dq, weight_grad = head_backward(jnp.concatenate(dq_blocks[h][::-1], axis=0), unit, scale, q_weights[h], cos_t, sin_t)
        put(width + h * dim, dq)
        qkv_acc[h * dim:(h + 1) * dim, :] += dot_nn(dq.T, n_rows)
        wn_ref[h:h + 1, :] += weight_grad
    dk, weight_grad = head_backward(k_acc[...] * score_scale, k_unit, k_scale, k_weight, cos_t, sin_t)
    wn_ref[heads:heads + 1, :] += weight_grad
    dv = v_acc[...].astype(BF16)
    put(2 * width, dk)
    put(2 * width + dim, dv)
    qkv_acc[width:width + dim, :] += dot_nn(dk.T, n_rows)
    qkv_acc[width + dim:width + 2 * dim, :] += dot_nn(dv.T, n_rows)


def front_kernel(n_ref, dy_ref, wg_ref, wu_ref, wd_ref, rope_ref, wq_ref, wk_ref, wv_ref, wo_ref, qn_ref, kn_ref,
                 m_ref, dn_ref, gn_ref, gdy_ref, mix_ref, wn_ref, packed_ref,
                 n_all, dy_all, rope_all, m_acc, k_acc, v_acc, qkv_acc, o_acc, send_sem, recv_sem, rope_send, rope_recv, out_sem, *, count, blocks, heads, dim):
    step = pl.program_id(0)
    me = lax.axis_index('sp')
    right, left, across, partner = lax.rem(me + 2, count), lax.rem(me + count - 2, count), lax.rem(me + 4, count), me + 1 - 2 * lax.rem(me, 2)
    other = lambda device: device + 1 - 2 * lax.rem(device, 2)
    batch, _, piece, model = n_all.shape

    def send(seq, index, src, into, slot, target):
        return pltpu.make_async_remote_copy(src_ref=src, dst_ref=into.at[seq, slot], send_sem=send_sem.at[seq, index], recv_sem=recv_sem.at[seq, index],
                                            device_id={'sp': target}, device_id_type=MESH)

    def forward(seq, index, ref, slot, target):
        return send(seq, index, ref.at[seq, slot], ref, slot, target)

    def own(seq):
        rows = pl.ds(pl.multiple_of(seq * piece, piece), piece)
        n, dy = n_ref.at[rows], dy_ref.at[rows]
        return [send(seq, 0, dy, dy_all, me, right), send(seq, 2, n, n_all, me, left), send(seq, 1, n, n_all, me, right),
                send(seq, 3, dy, dy_all, me, left), send(seq, 4, n, n_all, me, partner), send(seq, 5, dy, dy_all, me, partner)]

    def early(seq):
        return [forward(seq, 6, dy_all, left, right), forward(seq, 8, dy_all, left, partner), forward(seq, 7, n_all, right, left), forward(seq, 9, n_all, right, partner)]

    def late(seq):
        return [forward(seq, 10, n_all, left, partner), forward(seq, 11, dy_all, right, partner),
                forward(seq, 12, dy_all, across, partner), forward(seq, 13, n_all, across, partner)]

    def arrived(seq, index, ref, slot):
        send(seq, index, ref.at[seq, slot], ref, slot, partner).wait_recv()

    def start_own(seq):
        for copy in own(seq):
            copy.start()

    def pass_early(seq):
        copies = early(seq)
        arrived(seq, 0, dy_all, left)
        copies[0].start()
        copies[1].start()
        arrived(seq, 2, n_all, right)
        copies[2].start()
        copies[3].start()

    def pass_late(seq):
        for copy, (index, ref, slot) in zip(late(seq), ((1, n_all, left), (3, dy_all, right), (6, dy_all, across), (7, n_all, across))):
            arrived(seq, index, ref, slot)
            copy.start()

    def complete(seq):
        for index, ref, slot in ((4, n_all, partner), (5, dy_all, partner), (8, dy_all, other(left)), (9, n_all, other(right)),
                                 (10, n_all, other(left)), (11, dy_all, other(right)), (12, dy_all, other(across)), (13, n_all, other(across))):
            arrived(seq, index, ref, slot)

    def tables():
        return [pltpu.make_async_remote_copy(src_ref=rope_ref, dst_ref=rope_all.at[me], send_sem=rope_send.at[i], recv_sem=rope_recv.at[i],
                                             device_id={'sp': device}, device_id_type=MESH) for i, device in enumerate(other_devices(count))]

    def to_memory(seq):
        return [pltpu.make_async_copy(n_all.at[seq], gn_ref.at[seq], out_sem.at[seq, 0]), pltpu.make_async_copy(dy_all.at[seq], gdy_ref.at[seq], out_sem.at[seq, 1])]

    @pl.when(step == 0)
    def _():
        meet(count)
        start_own(0)
        for copy in tables():
            copy.start()
        start_own(1)
        for seq in range(batch):
            rows = slice(seq * piece, (seq + 1) * piece)
            n_all[seq, pl.ds(me, 1)] = n_ref[rows, :][None]
            dy_all[seq, pl.ds(me, 1)] = dy_ref[rows, :][None]
        rope_all[pl.ds(me, 1)] = rope_ref[...][None]
        wn_ref[...] = jnp.zeros_like(wn_ref)
        qkv_acc[...] = jnp.zeros_like(qkv_acc)
        o_acc[...] = jnp.zeros_like(o_acc)

    @pl.when(step == 2)
    def _():
        pass_early(0)

    @pl.when(step == 3)
    def _():
        start_own(2)

    @pl.when(step == blocks - 1)
    def _():
        pass_early(1)
        pass_late(0)

    @pl.when(step < blocks)
    def _():
        n, dy = n_ref[...], dy_ref[...]
        wg, wu, wd = wg_ref[...], wu_ref[...], wd_ref[...]
        hidden, d_gate, d_up = swiglu_both(dot_nn(n, wg), dot_nn(n, wu), dot_nt(dy, wd))
        m_new = dot_nn(hidden, wd)
        dn_new = dot_nt(d_gate, wg) + dot_nt(d_up, wu)

        @pl.when(step == 0)
        def _():
            m_acc[...] = m_new
            dn_ref[...] = dn_new

        @pl.when(step > 0)
        def _():
            m_acc[...] += m_new
            dn_ref[...] += dn_new

        @pl.when(step == blocks - 1)
        def _():
            m_ref[...] = m_acc[...].astype(BF16)

    @pl.when(step == blocks)
    def _():
        for copy in tables():
            copy.wait()

    @pl.when(step >= blocks)
    def _():
        seq = step - blocks

        @pl.when(seq + 3 < batch)
        def _():
            start_own(seq + 3)

        @pl.when(seq + 1 < batch)
        def _():
            pass_late(seq + 1)

        complete(seq)
        for copy in to_memory(seq):
            copy.start()
        full = count * piece
        one_sequence(me, n_all[seq].reshape(full, model), dy_all[seq].reshape(full, model), rope_all[:, 0].reshape(full, dim), rope_all[:, 1].reshape(full, dim),
                     wq_ref, wk_ref, wv_ref, wo_ref, qn_ref, kn_ref, mix_ref, wn_ref, k_acc, v_acc, qkv_acc, o_acc, heads, dim, min(128, full))

        @pl.when(seq + 2 < batch)
        def _():
            pass_early(seq + 2)

    @pl.when(step == pl.num_programs(0) - 1)
    def _():
        qkv_size = qkv_acc.shape[0]
        size = o_acc.shape[0]
        packed_ref[:, :qkv_size] = qkv_acc[...].T.astype(BF16)
        for i in range(model // size):
            packed_ref[i * size:(i + 1) * size, qkv_size:] = o_acc[:, i * size:(i + 1) * size].astype(BF16)

        @pl.loop(0, batch)
        def _(seq):
            for copy in own(seq) + early(seq) + late(seq):
                copy.wait_send()
            for copy in to_memory(seq):
                copy.wait()


def front(n, dy, w_gate, w_up, w_down, rope, w_q, w_k, w_v, w_o, q_norm, k_norm, count, piece, block):
    rows, model = n.shape
    ffn = w_gate.shape[1]
    num_heads, dim = q_norm.shape
    heads = num_heads // k_norm.shape[0]
    batch = rows // piece
    blocks = ffn // block
    width = (2 * heads + 2) * dim
    one = pl.Buffered(1)
    whole = lambda shape: pl.BlockSpec(shape, lambda i: (0,) * len(shape), pipeline_mode=one)
    cols = pl.BlockSpec((model, block), lambda i: (0, jnp.minimum(i, blocks - 1)))
    mine = lambda size: pl.BlockSpec((model, size), lambda i: (0, lax.axis_index('sp')), pipeline_mode=one)
    away = pl.BlockSpec(memory_space=pl.ANY)
    dma = pltpu.SemaphoreType.DMA
    vmem = pltpu.VMEM
    shape = jax.ShapeDtypeStruct
    return pl.pallas_call(
        functools.partial(front_kernel, count=count, blocks=blocks, heads=heads, dim=dim),
        grid=(blocks + batch,),
        in_specs=[whole((rows, model)), whole((rows, model)), cols, cols, pl.BlockSpec((block, model), lambda i: (jnp.minimum(i, blocks - 1), 0)), whole(rope.shape),
                  mine(heads * dim), mine(dim), mine(dim), pl.BlockSpec((heads * dim, model), lambda i: (lax.axis_index('sp'), 0), pipeline_mode=one),
                  whole(q_norm.shape), whole(k_norm.shape)],
        out_specs=[whole((rows, model)), whole((rows, model)), away, away,
                   pl.BlockSpec((count, 1, piece, width), lambda i: (0, jnp.maximum(i - blocks, 0), 0, 0)), whole((8, dim)), whole((model, width))],
        out_shape=[shape((rows, model), BF16), shape((rows, model), F32), shape((batch, count, piece, model), BF16), shape((batch, count, piece, model), BF16),
                   shape((count, batch, piece, width), BF16), shape((8, dim), F32), shape((model, width), BF16)],
        scratch_shapes=[vmem((batch, count, piece, model), BF16), vmem((batch, count, piece, model), BF16), vmem((count,) + rope.shape, F32), vmem((rows, model), F32),
                        vmem((count * piece, dim), F32), vmem((count * piece, dim), F32), vmem(((heads + 2) * dim, model), F32), vmem((heads * dim, model), F32),
                        dma((batch, 14)), dma((batch, 14)), dma((count - 1,)), dma((count - 1,)), dma((batch, 2))],
        compiler_params=pltpu.CompilerParams(vmem_limit_bytes=62 * 2 ** 20, collective_id=0, has_side_effects=True),
        cost_estimate=pl.CostEstimate(flops=12 * rows * model * ffn + 8 * batch * count * piece * model * width, bytes_accessed=6 * model * ffn, transcendentals=0),
    )(n, dy, w_gate, w_up, w_down, rope, w_q, w_k, w_v, w_o, q_norm, k_norm)


def norm_kernel(x_ref, gain_ref, n_ref):
    x = x_ref[...].astype(F32)
    centered = x - jnp.mean(x, axis=-1, keepdims=True)
    scale = lax.rsqrt(jnp.mean(centered * centered, axis=-1, keepdims=True) + NORM_EPS)
    n_ref[...] = (centered * scale * gain_ref[...]).astype(BF16)


def input_norm(x, gain):
    rows, model = x.shape
    tile = rows // 4
    return pl.pallas_call(
        norm_kernel,
        grid=(rows // tile,),
        in_specs=[pl.BlockSpec((tile, model), lambda i: (i, 0)), pl.BlockSpec((1, model), lambda i: (0, 0))],
        out_specs=pl.BlockSpec((tile, model), lambda i: (i, 0)),
        out_shape=jax.ShapeDtypeStruct((rows, model), BF16),
        cost_estimate=pl.CostEstimate(flops=8 * rows * model, bytes_accessed=4 * rows * model, transcendentals=0),
    )(x, gain)


def finish_kernel(core_ref, mix_ref, x_ref, dy_ref, m_ref, dn_ref, gain_ref, wq_ref, wk_ref, wv_ref, wo_ref, gg_ref, gu_ref, gd_ref, pg_ref, pu_ref, pd_ref,
                  y_ref, dx_ref, gain_grad_ref, fg_ref, fu_ref, fd_ref, a_acc, d_acc, col_buf, row_buf, in_sem, out_sem, *, parts):
    step = pl.program_id(0)
    steps = pl.num_programs(0)
    o_size, k_size = parts
    share = gg_ref.shape[1]
    slots, _, col_rows, _ = col_buf.shape
    row_rows = row_buf.shape[2]
    mine, theirs = pl.multiple_of(core_ref[0] * share, share), pl.multiple_of((1 - core_ref[0]) * share, share)

    def fetches(at):
        slot = lax.rem(at, slots)
        cols = pl.ds(pl.multiple_of(at * col_rows, col_rows), col_rows)
        rows = pl.ds(pl.multiple_of(at * row_rows, row_rows), row_rows)
        pairs = [(ref.at[cols], col_buf.at[slot, i]) for i, ref in enumerate((gg_ref, gu_ref, pg_ref, pu_ref))]
        pairs += [(ref.at[rows], row_buf.at[slot, i]) for i, ref in enumerate((gd_ref, pd_ref))]
        return [pltpu.make_async_copy(src, dst, in_sem.at[slot, i]) for i, (src, dst) in enumerate(pairs)]

    def places(at):
        slot = lax.rem(at, slots)
        cols = pl.ds(pl.multiple_of(at * col_rows, col_rows), col_rows)
        pairs = [(col_buf.at[slot, i], ref.at[cols, pl.ds(start, share)]) for i, (ref, start) in enumerate(((fg_ref, mine), (fu_ref, mine), (fg_ref, theirs), (fu_ref, theirs)))]
        pairs += [(row_buf.at[slot, i], fd_ref.at[pl.ds(pl.multiple_of(start + at * row_rows, row_rows), row_rows)]) for i, start in enumerate((mine, theirs))]
        return [pltpu.make_async_copy(src, dst, out_sem.at[slot, i]) for i, (src, dst) in enumerate(pairs)]

    @pl.when(step == 0)
    def _():
        for copy in fetches(0):
            copy.start()

    @pl.when(step > 1)
    def _():
        for copy in places(step - 2):
            copy.wait()

    @pl.when(step < steps - 1)
    def _():
        for copy in fetches(step + 1):
            copy.start()

    mix = mix_ref[0]
    a_new = dot_nn(mix[:, :o_size], wo_ref[...])
    d_new = dot_nt(mix[:, o_size:2 * o_size], wq_ref[...])
    d_new += dot_nt(mix[:, 2 * o_size:2 * o_size + k_size], wk_ref[...]) + dot_nt(mix[:, 2 * o_size + k_size:], wv_ref[...])

    @pl.when(step == 0)
    def _():
        a_acc[...] = a_new
        d_acc[...] = d_new + dn_ref[...]

    @pl.when(step > 0)
    def _():
        a_acc[...] += a_new
        d_acc[...] += d_new

    for copy in fetches(step):
        copy.wait()
    for copy in places(step):
        copy.start()

    @pl.when(step == steps - 1)
    def _():
        x = x_ref[...].astype(F32)
        y_ref[...] = (x + a_acc[...].astype(BF16).astype(F32) + m_ref[...].astype(F32)).astype(BF16)
        centered = x - jnp.mean(x, axis=-1, keepdims=True)
        scale = lax.rsqrt(jnp.mean(centered * centered, axis=-1, keepdims=True) + NORM_EPS)
        unit = centered * scale
        grad = d_acc[...].astype(BF16).astype(F32)
        gain_grad = jnp.sum(grad * unit, axis=0, keepdims=True)
        rows, lanes = gain_grad_ref.shape
        for i in range(rows):
            gain_grad_ref[i:i + 1, :] = gain_grad[:, i * lanes:(i + 1) * lanes]
        grad = grad * gain_ref[...]
        along = jnp.mean(grad * unit, axis=-1, keepdims=True)
        grad = scale * (grad - jnp.mean(grad, axis=-1, keepdims=True) - unit * along)
        dx_ref[...] = (dy_ref[...].astype(F32) + grad).astype(BF16)
        for copy in places(step - 1) + places(step):
            copy.wait()


def finish(core, mix, x, dy, mlp_out, d_norm, gain, w_q, w_k, w_v, w_o, own_grads, partner_grads, o_size, k_size):
    rows, model = x.shape
    pieces, _, width = mix.shape
    share = own_grads[0].shape[1]
    whole = pl.BlockSpec((rows, model), lambda i, c: (0, 0))
    row = pl.BlockSpec((1, model), lambda i, c: (0, 0))
    gain_shape = (model // k_size, k_size)
    cols = lambda size: pl.BlockSpec((model, size), lambda i, c: (0, i))
    away = pl.BlockSpec(memory_space=pl.ANY)
    bf16 = lambda *shape: jax.ShapeDtypeStruct(shape, BF16)
    return pl.pallas_call(
        functools.partial(finish_kernel, parts=(o_size, k_size)),
        grid_spec=pltpu.PrefetchScalarGridSpec(
            num_scalar_prefetch=1,
            grid=(pieces,),
            in_specs=[pl.BlockSpec((1, rows, width), lambda i, c: (i, 0, 0))] + [whole] * 4
            + [row, cols(o_size), cols(k_size), cols(k_size), pl.BlockSpec((o_size, model), lambda i, c: (i, 0))] + [away] * 6,
            out_specs=[whole, whole, pl.BlockSpec(gain_shape, lambda i, c: (0, 0))] + [away] * 3,
            scratch_shapes=[pltpu.VMEM((rows, model), F32), pltpu.VMEM((rows, model), F32),
                            pltpu.VMEM((3, 4, model // pieces, share), BF16), pltpu.VMEM((3, 2, share // pieces, model), BF16),
                            pltpu.SemaphoreType.DMA((3, 6)), pltpu.SemaphoreType.DMA((3, 6))],
        ),
        out_shape=[bf16(rows, model), bf16(rows, model), jax.ShapeDtypeStruct(gain_shape, F32)]
        + [bf16(model, 2 * share), bf16(model, 2 * share), bf16(2 * share, model)],
        compiler_params=pltpu.CompilerParams(vmem_limit_bytes=56 * 2 ** 20),
        cost_estimate=pl.CostEstimate(flops=2 * pieces * rows * width * model, bytes_accessed=14 * rows * model + 2 * pieces * width * (rows + model), transcendentals=0),
    )(core, mix, x, dy, mlp_out, d_norm, gain, w_q, w_k, w_v, w_o, *own_grads, *partner_grads)


def place_kernel(packed_ref, fq_ref, fk_ref, fv_ref, fo_ref, buf, in_sem, out_sem, *, o_size, k_size):
    count, model, _ = packed_ref.shape
    fetch = lambda at: pltpu.make_async_copy(packed_ref.at[at], buf.at[at], in_sem.at[at])

    def places(at):
        part = buf.at[at]
        pairs = [(part.at[:, pl.ds(0, o_size)], fq_ref.at[:, pl.ds(at * o_size, o_size)]), (part.at[:, pl.ds(o_size, k_size)], fk_ref.at[:, pl.ds(at * k_size, k_size)]),
                 (part.at[:, pl.ds(o_size + k_size, k_size)], fv_ref.at[:, pl.ds(at * k_size, k_size)])]
        pairs += [(part.at[pl.ds(i * o_size, o_size), pl.ds(o_size + 2 * k_size, o_size)], fo_ref.at[pl.ds(at * o_size, o_size), pl.ds(i * o_size, o_size)])
                  for i in range(model // o_size)]
        return [pltpu.make_async_copy(src, dst, out_sem.at[at, i]) for i, (src, dst) in enumerate(pairs)]

    for at in range(count):
        fetch(at).start()
    for at in range(count):
        fetch(at).wait()
        for copy in places(at):
            copy.start()
    for at in range(count):
        for copy in places(at):
            copy.wait()


def place(packed, weights, o_size, k_size):
    count, model, _ = packed.shape
    away = pl.BlockSpec(memory_space=pl.ANY)
    return pl.pallas_call(
        functools.partial(place_kernel, o_size=o_size, k_size=k_size),
        in_specs=[away],
        out_specs=[away] * 4,
        out_shape=[jax.ShapeDtypeStruct(weight.shape, BF16) for weight in weights],
        scratch_shapes=[pltpu.VMEM(packed.shape, BF16), pltpu.SemaphoreType.DMA((count,)), pltpu.SemaphoreType.DMA((count, 3 + model // o_size))],
        compiler_params=pltpu.CompilerParams(vmem_limit_bytes=40 * 2 ** 20),
        cost_estimate=pl.CostEstimate(flops=2 ** 20, bytes_accessed=4 * packed.size, transcendentals=0),
    )(packed)


def share_kernel(gain_ref, norm_ref, gain_out, q_out, k_out, parts, send_sem, recv_sem, *, count, heads):
    me = lax.axis_index('sp')
    rows = gain_ref.shape[0]
    meet(count)
    copies = [pltpu.make_async_remote_copy(src_ref=src, dst_ref=parts.at[me, pl.ds(j * rows, rows)], send_sem=send_sem.at[i, j], recv_sem=recv_sem.at[i, j],
                                           device_id={'sp': device}, device_id_type=MESH)
              for i, device in enumerate(other_devices(count)) for j, src in enumerate((gain_ref, norm_ref))]
    for copy in copies:
        copy.start()
    parts[pl.ds(me, 1), :rows] = gain_ref[...][None]
    parts[pl.ds(me, 1), rows:] = norm_ref[...][None]
    for copy in copies:
        copy.wait()
    gain_out[...] = jnp.sum(parts[:, :rows], axis=0)
    for device in range(count):
        q_out[device * heads:(device + 1) * heads, :] = parts[device, rows:rows + heads, :]
        k_out[device:device + 1, :] = parts[device, rows + heads:rows + heads + 1, :]


def share_small(gain, norms, q_norm, k_norm, count):
    vmem = pl.BlockSpec(memory_space=pltpu.VMEM)
    heads = q_norm.shape[0] // k_norm.shape[0]
    dma = pltpu.SemaphoreType.DMA((count - 1, 2))
    return pl.pallas_call(
        functools.partial(share_kernel, count=count, heads=heads),
        in_specs=[vmem] * 2,
        out_specs=[vmem] * 3,
        out_shape=[jax.ShapeDtypeStruct(part.shape, F32) for part in (gain, q_norm, k_norm)],
        scratch_shapes=[pltpu.VMEM((count, 2 * gain.shape[0], gain.shape[1]), F32), dma, dma],
        compiler_params=pltpu.CompilerParams(collective_id=2, has_side_effects=True),
    )(gain, norms)


def solution(mesh):
    n_sp = mesh.shape['sp']
    seq_spec = P('dp', 'sp', None)
    grad_spec = P('dp', None)

    def layer_step(x_in, grad_y, positions, w_q, w_k, w_v, w_o, w_gate, w_up, w_down, norm_gain, q_norm, k_norm):
        batch, piece, model = x_in.shape
        num_heads, dim = q_norm.shape
        heads = num_heads // k_norm.shape[0]
        ffn = w_gate.shape[1]
        tokens = batch * piece
        me = lax.axis_index('sp')
        gain_row = norm_gain.reshape(1, model)
        x_rows, dy_own = x_in.reshape(tokens, model), grad_y.reshape(tokens, model)
        n_own = input_norm(x_rows, gain_row)

        inv_freq = ROPE_THETA ** (-(jnp.arange(dim // 2, dtype=F32) * 2.0) / dim)
        angles = jnp.repeat(positions.astype(F32)[:, None] * inv_freq[None, :], 2, axis=1)
        sign = jnp.where(jnp.arange(dim) % 2 == 0, -1.0, 1.0).astype(F32)
        rope_own = jnp.stack([jnp.cos(angles), jnp.sin(angles) * sign[None, :]])

        mlp_out, d_norm, n_all, dy_all, mix, norm_grads, packed = front(n_own, dy_own, w_gate, w_up, w_down, rope_own, w_q, w_k, w_v, w_o, q_norm, k_norm,
                                                                        n_sp, piece, ffn // 6)
        packed = lax.all_gather(packed, 'sp', axis=0, tiled=False)

        by_tile = lambda part: part.reshape(n_sp, -1, part.shape[-1])
        *grads, mix = all_mlp([(by_tile(n_all), 0)], [(by_tile(dy_all), 0)], w_gate, w_up, w_down, by_tile(mix), ffn // 6)

        y_out, grad_x, grad_gain, full_gate, full_up, full_down = finish((me % 2).reshape(1), mix, x_rows, dy_own, mlp_out, d_norm, gain_row, w_q, w_k, w_v, w_o,
                                                                         grads[:3], grads[3:], heads * dim, dim)
        full_gain, full_qn, full_kn = share_small(grad_gain, norm_grads, q_norm, k_norm, n_sp)
        packed, full_gain = lax.optimization_barrier((packed, full_gain))
        full_q, full_k, full_v, full_o = place(packed, (w_q, w_k, w_v, w_o), heads * dim, dim)
        return (y_out.reshape(x_in.shape), grad_x.reshape(x_in.shape), full_q, full_k, full_v, full_o, full_gate, full_up, full_down,
                full_gain.reshape(model), full_qn, full_kn)

    in_specs = (seq_spec, seq_spec, P(('dp', 'sp'))) + (P(),) * 10
    out_specs = (seq_spec, seq_spec) + (grad_spec,) * 7 + (P('dp'), grad_spec, grad_spec)
    return jax.shard_map(layer_step, mesh=mesh, in_specs=in_specs, out_specs=out_specs, check_vma=False)
```

```python
import functools

import jax
import jax.numpy as jnp
from jax import lax
from jax.experimental import pallas as pl
from jax.experimental.pallas import tpu as pltpu
from jax.sharding import PartitionSpec as P

NORM_EPS = 1e-5
ROPE_THETA = 75.0e6
F32 = jnp.float32
BF16 = jnp.bfloat16
MESH = pl.DeviceIdType.MESH


def dot_nn(lhs, rhs):
    return lax.dot_general(lhs, rhs, (((1,), (0,)), ((), ())), preferred_element_type=F32)


def dot_nt(lhs, rhs):
    return lax.dot_general(lhs, rhs, (((1,), (1,)), ((), ())), preferred_element_type=F32)


def swiglu_both(gate, up, d_hidden):
    sig = jax.nn.sigmoid(gate)
    act = gate * sig
    d_hidden = d_hidden.astype(BF16).astype(F32)
    d_gate = d_hidden * up * (sig * (1.0 + gate * (1.0 - sig)))
    return (act * up).astype(BF16), d_gate.astype(BF16), (d_hidden * act).astype(BF16)


def other_devices(count):
    me = lax.axis_index('sp')
    return [lax.rem(me + shift, count) for shift in range(1, count)]


def meet(count):
    barrier = pltpu.get_barrier_semaphore()
    for device in other_devices(count):
        pl.semaphore_signal(barrier, inc=1, device_id={'sp': device}, device_id_type=MESH)
    pl.semaphore_wait(barrier, count - 1)


def all_mlp_kernel(n_ref, dy_ref, wg_ref, wu_ref, wd_ref, mix_ref, qk_ref, vo_ref, gg_ref, gu_ref, gd_ref, pg_ref, pu_ref, pd_ref, swap_ref, qk_all, vo_all,
                   n_t, dy_t, acc_g, acc_u, acc_d, swap_send, swap_recv, half_send, half_recv, ring_send, ring_recv, own_sem, *, block, count):
    step = pl.program_id(0)
    last = pl.num_programs(0) - 1
    share = wg_ref.shape[1]
    me = lax.axis_index('sp')
    right, left, across, partner = lax.rem(me + 2, count), lax.rem(me + count - 2, count), lax.rem(me + 4, count), me + 1 - 2 * lax.rem(me, 2)
    other = lambda device: device + 1 - 2 * lax.rem(device, 2)

    def swaps(shifts):
        copies = []
        for shift in shifts:
            device = lax.rem(me + shift, count)
            copies.append(pltpu.make_async_remote_copy(src_ref=mix_ref.at[device], dst_ref=swap_ref.at[me], send_sem=swap_send.at[shift - 1], recv_sem=swap_recv.at[shift - 1],
                                                       device_id={'sp': device}, device_id_type=MESH))
        return copies

    near = [1, count - 1, 2, count - 2]
    far = [shift for shift in range(3, count - 2)]

    def halves(i):
        cols = pl.ds(i * block, block)
        return [pltpu.make_async_remote_copy(src_ref=src.at[index], dst_ref=dst.at[index], send_sem=half_send.at[i, j], recv_sem=half_recv.at[i, j],
                                             device_id={'sp': partner}, device_id_type=MESH)
                for j, (src, dst, index) in enumerate(((gg_ref, pg_ref, (slice(None), cols)), (gu_ref, pu_ref, (slice(None), cols)), (gd_ref, pd_ref, (cols,))))]

    def send(index, src, into, slot, target):
        return pltpu.make_async_remote_copy(src_ref=src, dst_ref=into.at[slot], send_sem=ring_send.at[index], recv_sem=ring_recv.at[index],
                                            device_id={'sp': target}, device_id_type=MESH)

    def forward(index, ref, slot, target):
        return send(index, ref.at[slot], ref, slot, target)

    def arrived(index, ref, slot):
        send(index, ref.at[slot], ref, slot, partner).wait_recv()

    own = lambda: [send(0, vo_ref, vo_all, me, right), send(2, qk_ref, qk_all, me, left), send(1, qk_ref, qk_all, me, right),
                   send(3, vo_ref, vo_all, me, left), send(4, qk_ref, qk_all, me, partner), send(5, vo_ref, vo_all, me, partner)]
    early = lambda: [forward(6, vo_all, left, right), forward(7, qk_all, right, left), forward(8, vo_all, left, partner), forward(9, qk_all, right, partner)]
    late = lambda: [forward(10, qk_all, left, partner), forward(11, vo_all, right, partner), forward(12, vo_all, across, partner), forward(13, qk_all, across, partner)]
    keep = lambda: [pltpu.make_async_copy(mix_ref.at[me], swap_ref.at[me], own_sem.at[0]), pltpu.make_async_copy(qk_ref, qk_all.at[me], own_sem.at[1]),
                    pltpu.make_async_copy(vo_ref, vo_all.at[me], own_sem.at[2])]

    @pl.when(step == 0)
    def _():
        meet(count)
        for copy in own() + swaps(near) + keep():
            copy.start()
        acc_g[...] = jnp.zeros_like(acc_g)
        acc_u[...] = jnp.zeros_like(acc_u)
        acc_d[...] = jnp.zeros_like(acc_d)

    @pl.when(step == last // 2)
    def _():
        arrived(0, vo_all, left)
        arrived(2, qk_all, right)
        for copy in early() + swaps(far):
            copy.start()

    n_t[...] = n_ref[0].T
    dy_t[...] = dy_ref[0].T

    @pl.loop(0, share // block)
    def _(i):
        cols = pl.ds(pl.multiple_of(i * block, block), block)
        n, dy = n_ref[0], dy_ref[0]
        hidden, d_gate, d_up = swiglu_both(dot_nn(n, wg_ref[:, cols]), dot_nn(n, wu_ref[:, cols]), dot_nt(dy, wd_ref[cols, :]))
        acc_g[:, cols] += dot_nn(n_t[...], d_gate)
        acc_u[:, cols] += dot_nn(n_t[...], d_up)
        acc_d[:, cols] += dot_nn(dy_t[...], hidden)

        @pl.when(step == last)
        def _():
            gg_ref[:, cols] = acc_g[:, cols].astype(BF16)
            gu_ref[:, cols] = acc_u[:, cols].astype(BF16)
            gd_ref[cols, :] = acc_d[:, cols].T.astype(BF16)

        for done in range(share // block - 1):
            @pl.when((step == last) & (i == done + 1))
            def _():
                for copy in halves(done):
                    copy.start()

    @pl.when(step == last)
    def _():
        arrived(1, qk_all, left)
        arrived(3, vo_all, right)
        late_copies = late()
        late_copies[0].start()
        late_copies[1].start()
        for copy in halves(share // block - 1):
            copy.start()
        arrived(6, vo_all, across)
        late_copies[2].start()
        arrived(7, qk_all, across)
        late_copies[3].start()
        for index, ref, slot in ((4, qk_all, partner), (5, vo_all, partner), (8, vo_all, other(left)), (9, qk_all, other(right)),
                                 (10, qk_all, other(left)), (11, vo_all, other(right)), (12, vo_all, other(across)), (13, qk_all, other(across))):
            arrived(index, ref, slot)
        for copy in own() + early() + late_copies:
            copy.wait_send()
        for copy in swaps(near + far):
            copy.wait()
        for copy in keep():
            copy.wait()
        for i in range(share // block):
            for copy in halves(i):
                copy.wait()


def all_mlp(n, dy, w_gate, w_up, w_down, mix, qk, vo, block):
    count, tile, model = n.shape
    share = w_gate.shape[1] // 2
    tok = pl.BlockSpec((1, tile, model), lambda i: (i, 0, 0))
    one = pl.Buffered(1)
    core = lambda: lax.rem(lax.axis_index('sp'), 2)
    in_cols = pl.BlockSpec((model, share), lambda i: (0, core()), pipeline_mode=one)
    out_cols = pl.BlockSpec((model, share), lambda i: (0, 0), pipeline_mode=one)
    away = pl.BlockSpec(memory_space=pl.ANY)
    dma = pltpu.SemaphoreType.DMA
    shape = lambda *dims: jax.ShapeDtypeStruct(dims, BF16)
    grads = [shape(model, share), shape(model, share), shape(share, model)]
    return pl.pallas_call(
        functools.partial(all_mlp_kernel, block=block, count=count),
        grid=(count,),
        in_specs=[tok, tok, in_cols, in_cols, pl.BlockSpec((share, model), lambda i: (core(), 0), pipeline_mode=one), away, away, away],
        out_specs=[out_cols, out_cols, pl.BlockSpec((share, model), lambda i: (0, 0), pipeline_mode=one)] + [away] * 6,
        out_shape=grads + grads + [shape(*mix.shape), shape(count, *qk.shape), shape(count, *vo.shape)],
        scratch_shapes=[pltpu.VMEM((model, tile), BF16)] * 2 + [pltpu.VMEM((model, share), F32)] * 3
        + [dma((count - 1,)), dma((count - 1,)), dma((share // block, 3)), dma((share // block, 3)), dma((14,)), dma((14,)), dma((3,))],
        compiler_params=pltpu.CompilerParams(vmem_limit_bytes=61 * 2 ** 20, collective_id=1, has_side_effects=True),
        cost_estimate=pl.CostEstimate(flops=12 * count * tile * model * share, bytes_accessed=4 * model * count * tile + 12 * model * share, transcendentals=0),
    )(n, dy, w_gate, w_up, w_down, mix, qk, vo)


def swap_pairs(rows):
    width = rows.shape[1]
    lane = lax.broadcasted_iota(jnp.int32, rows.shape, 1)
    return jnp.where(lane % 2 == 0, pltpu.roll(rows, width - 1, 1), pltpu.roll(rows, 1, 1))


def head_forward(rows, weight, cos_t, sin_t):
    rows = rows.astype(F32)
    centered = rows - jnp.mean(rows, axis=-1, keepdims=True)
    scale = lax.rsqrt(jnp.mean(centered * centered, axis=-1, keepdims=True) + NORM_EPS)
    unit = centered * scale
    normed = unit * weight
    return (normed * cos_t + swap_pairs(normed) * sin_t).astype(BF16), unit, scale


def head_backward(grad, unit, scale, weight, cos_t, sin_t):
    grad = grad.astype(BF16).astype(F32)
    grad = grad * cos_t - swap_pairs(grad) * sin_t
    weight_grad = jnp.sum(grad * unit, axis=0, keepdims=True)
    grad = grad * weight
    along = jnp.mean(grad * unit, axis=-1, keepdims=True)
    grad = scale * (grad - jnp.mean(grad, axis=-1, keepdims=True) - unit * along)
    return grad.astype(BF16), weight_grad


def one_sequence(me, n_rows, dy_rows, cos_t, sin_t, wq_ref, wk_ref, wv_ref, wo_ref, qn_ref, kn_ref, mix_ref, wn_ref, k_acc, v_acc, qkv_acc, o_acc, heads, dim, block):
    pieces, _, piece, _ = mix_ref.shape
    full = pieces * piece
    score_scale = dim ** -0.5
    width = heads * dim

    def put(start, rows):
        mix_ref[:, 0, :, start:start + rows.shape[1]] = rows.reshape(pieces, piece, rows.shape[1])

    q_proj = dot_nn(n_rows, wq_ref[...]).astype(BF16)
    k_proj = dot_nn(n_rows, wk_ref[...]).astype(BF16)
    v_rows = dot_nn(n_rows, wv_ref[...]).astype(BF16)
    d_out = dot_nt(dy_rows, wo_ref[...]).astype(BF16)
    q_weights = [qn_ref[pl.ds(me * heads + h, 1), :] for h in range(heads)]
    k_weight = kn_ref[pl.ds(me, 1), :]
    q_parts = [head_forward(q_proj[:, h * dim:(h + 1) * dim], q_weights[h], cos_t, sin_t) for h in range(heads)]
    k_rot, k_unit, k_scale = head_forward(k_proj, k_weight, cos_t, sin_t)
    k_t, v_t = k_rot.T, v_rows.T
    o_blocks, dq_blocks = [[] for _ in range(heads)], [[] for _ in range(heads)]
    for start in range(full - block, -1, -block):
        stop = start + block
        q_blk = jnp.concatenate([q_parts[h][0][start:stop] for h in range(heads)], axis=0)
        do_blk = jnp.concatenate([d_out[start:stop, h * dim:(h + 1) * dim] for h in range(heads)], axis=0)
        k_blk, v_blk = k_rot[:stop], v_rows[:stop]
        scores = dot_nt(k_blk, q_blk)
        tail = scores[start:]
        key = lax.broadcasted_iota(jnp.int32, tail.shape, 0)
        query = lax.broadcasted_iota(jnp.int32, tail.shape, 1) % block
        tail = jnp.where(query >= key, tail, -1e30)
        scores = tail if start == 0 else jnp.concatenate([scores[:start], tail], axis=0)
        top = jnp.max(scores, axis=0, keepdims=True)
        probs = jnp.exp((scores - top) * score_scale)
        probs = probs * (1.0 / jnp.sum(probs, axis=0, keepdims=True))
        probs_b = probs.astype(BF16)
        o_blk = dot_nn(v_t[:, :stop], probs_b).astype(BF16)
        d_probs = dot_nt(v_blk, do_blk)
        delta = jnp.sum(probs * d_probs, axis=0, keepdims=True)
        d_scores = (probs * (d_probs - delta)).astype(BF16)
        dq_blk = dot_nn(k_t[:, :stop], d_scores) * score_scale
        dk_new, dv_new = dot_nn(d_scores, q_blk), dot_nn(probs_b, do_blk)
        if stop == full:
            k_acc[...], v_acc[...] = dk_new, dv_new
        else:
            k_acc[0:stop, :] += dk_new
            v_acc[0:stop, :] += dv_new
        for h in range(heads):
            o_blocks[h].append(o_blk[:, h * block:(h + 1) * block])
            dq_blocks[h].append(dq_blk[:, h * block:(h + 1) * block].T)
    for h in range(heads):
        o_t = jnp.concatenate(o_blocks[h][::-1], axis=1)
        put(h * dim, o_t.T)
        o_acc[h * dim:(h + 1) * dim, :] += dot_nn(o_t, dy_rows)
        _, unit, scale = q_parts[h]
        dq, weight_grad = head_backward(jnp.concatenate(dq_blocks[h][::-1], axis=0), unit, scale, q_weights[h], cos_t, sin_t)
        put(width + h * dim, dq)
        qkv_acc[h * dim:(h + 1) * dim, :] += dot_nn(dq.T, n_rows)
        wn_ref[h:h + 1, :] += weight_grad
    dk, weight_grad = head_backward(k_acc[...] * score_scale, k_unit, k_scale, k_weight, cos_t, sin_t)
    wn_ref[heads:heads + 1, :] += weight_grad
    dv = v_acc[...].astype(BF16)
    put(2 * width, dk)
    put(2 * width + dim, dv)
    qkv_acc[width:width + dim, :] += dot_nn(dk.T, n_rows)
    qkv_acc[width + dim:width + 2 * dim, :] += dot_nn(dv.T, n_rows)


def front_kernel(n_ref, dy_ref, wg_ref, wu_ref, wd_ref, rope_ref, wq_ref, wk_ref, wv_ref, wo_ref, qn_ref, kn_ref,
                 m_ref, dn_ref, gn_ref, gdy_ref, mix_ref, wn_ref, qk_ref, vo_ref,
                 n_all, dy_all, rope_all, m_acc, k_acc, v_acc, qkv_acc, o_acc, send_sem, recv_sem, rope_send, rope_recv, out_sem, *, count, blocks, heads, dim):
    step = pl.program_id(0)
    me = lax.axis_index('sp')
    right, left, across, partner = lax.rem(me + 2, count), lax.rem(me + count - 2, count), lax.rem(me + 4, count), me + 1 - 2 * lax.rem(me, 2)
    other = lambda device: device + 1 - 2 * lax.rem(device, 2)
    batch, _, piece, model = n_all.shape

    def send(seq, index, src, into, slot, target):
        return pltpu.make_async_remote_copy(src_ref=src, dst_ref=into.at[seq, slot], send_sem=send_sem.at[seq, index], recv_sem=recv_sem.at[seq, index],
                                            device_id={'sp': target}, device_id_type=MESH)

    def forward(seq, index, ref, slot, target):
        return send(seq, index, ref.at[seq, slot], ref, slot, target)

    def own(seq):
        rows = pl.ds(pl.multiple_of(seq * piece, piece), piece)
        n, dy = n_ref.at[rows], dy_ref.at[rows]
        return [send(seq, 0, dy, dy_all, me, right), send(seq, 2, n, n_all, me, left), send(seq, 1, n, n_all, me, right),
                send(seq, 3, dy, dy_all, me, left), send(seq, 4, n, n_all, me, partner), send(seq, 5, dy, dy_all, me, partner)]

    def early(seq):
        return [forward(seq, 6, dy_all, left, right), forward(seq, 8, dy_all, left, partner), forward(seq, 7, n_all, right, left), forward(seq, 9, n_all, right, partner)]

    def late(seq):
        return [forward(seq, 10, n_all, left, partner), forward(seq, 11, dy_all, right, partner),
                forward(seq, 12, dy_all, across, partner), forward(seq, 13, n_all, across, partner)]

    def arrived(seq, index, ref, slot):
        send(seq, index, ref.at[seq, slot], ref, slot, partner).wait_recv()

    def start_own(seq):
        for copy in own(seq):
            copy.start()

    def pass_early(seq):
        copies = early(seq)
        arrived(seq, 0, dy_all, left)
        copies[0].start()
        copies[1].start()
        arrived(seq, 2, n_all, right)
        copies[2].start()
        copies[3].start()

    def pass_late(seq):
        for copy, (index, ref, slot) in zip(late(seq), ((1, n_all, left), (3, dy_all, right), (6, dy_all, across), (7, n_all, across))):
            arrived(seq, index, ref, slot)
            copy.start()

    def complete(seq):
        for index, ref, slot in ((4, n_all, partner), (5, dy_all, partner), (8, dy_all, other(left)), (9, n_all, other(right)),
                                 (10, n_all, other(left)), (11, dy_all, other(right)), (12, dy_all, other(across)), (13, n_all, other(across))):
            arrived(seq, index, ref, slot)

    def tables():
        return [pltpu.make_async_remote_copy(src_ref=rope_ref, dst_ref=rope_all.at[me], send_sem=rope_send.at[i], recv_sem=rope_recv.at[i],
                                             device_id={'sp': device}, device_id_type=MESH) for i, device in enumerate(other_devices(count))]

    def to_memory(seq):
        return [pltpu.make_async_copy(n_all.at[seq], gn_ref.at[seq], out_sem.at[seq, 0]), pltpu.make_async_copy(dy_all.at[seq], gdy_ref.at[seq], out_sem.at[seq, 1])]

    @pl.when(step == 0)
    def _():
        meet(count)
        start_own(0)
        for copy in tables():
            copy.start()
        start_own(1)
        for seq in range(batch):
            rows = slice(seq * piece, (seq + 1) * piece)
            n_all[seq, pl.ds(me, 1)] = n_ref[rows, :][None]
            dy_all[seq, pl.ds(me, 1)] = dy_ref[rows, :][None]
        rope_all[pl.ds(me, 1)] = rope_ref[...][None]
        wn_ref[...] = jnp.zeros_like(wn_ref)
        qkv_acc[...] = jnp.zeros_like(qkv_acc)
        o_acc[...] = jnp.zeros_like(o_acc)

    @pl.when(step == 2)
    def _():
        pass_early(0)
        start_own(2)

    @pl.when(step == blocks - 2)
    def _():
        pass_early(1)
        start_own(3)

    @pl.when(step == blocks - 1)
    def _():
        pass_late(0)

    @pl.when(step < blocks)
    def _():
        n, dy = n_ref[...], dy_ref[...]
        wg, wu, wd = wg_ref[...], wu_ref[...], wd_ref[...]
        hidden, d_gate, d_up = swiglu_both(dot_nn(n, wg), dot_nn(n, wu), dot_nt(dy, wd))
        m_new = dot_nn(hidden, wd)
        dn_new = dot_nt(d_gate, wg) + dot_nt(d_up, wu)

        @pl.when(step == 0)
        def _():
            m_acc[...] = m_new
            dn_ref[...] = dn_new

        @pl.when(step > 0)
        def _():
            m_acc[...] += m_new
            dn_ref[...] += dn_new

        @pl.when(step == blocks - 1)
        def _():
            m_ref[...] = m_acc[...].astype(BF16)

    @pl.when(step == blocks)
    def _():
        for copy in tables():
            copy.wait()

    @pl.when(step >= blocks)
    def _():
        seq = step - blocks

        @pl.when(seq + 2 < batch)
        def _():
            pass_early(seq + 2)

        @pl.when(seq + 4 < batch)
        def _():
            start_own(seq + 4)

        @pl.when(seq + 1 < batch)
        def _():
            pass_late(seq + 1)

        complete(seq)
        for copy in to_memory(seq):
            copy.start()
        full = count * piece
        one_sequence(me, n_all[seq].reshape(full, model), dy_all[seq].reshape(full, model), rope_all[:, 0].reshape(full, dim), rope_all[:, 1].reshape(full, dim),
                     wq_ref, wk_ref, wv_ref, wo_ref, qn_ref, kn_ref, mix_ref, wn_ref, k_acc, v_acc, qkv_acc, o_acc, heads, dim, min(128, full))

    @pl.when(step == pl.num_programs(0) - 1)
    def _():
        size = o_acc.shape[0]
        qk_size = size + dim
        qk_ref[...] = qkv_acc[:qk_size, :].T.astype(BF16)
        vo_ref[:, :dim] = qkv_acc[qk_size:, :].T.astype(BF16)
        for i in range(model // size):
            vo_ref[i * size:(i + 1) * size, dim:] = o_acc[:, i * size:(i + 1) * size].astype(BF16)

        @pl.loop(0, batch)
        def _(seq):
            for copy in own(seq) + early(seq) + late(seq):
                copy.wait_send()
            for copy in to_memory(seq):
                copy.wait()


def front(n, dy, w_gate, w_up, w_down, rope, w_q, w_k, w_v, w_o, q_norm, k_norm, count, piece, block):
    rows, model = n.shape
    ffn = w_gate.shape[1]
    num_heads, dim = q_norm.shape
    heads = num_heads // k_norm.shape[0]
    batch = rows // piece
    blocks = ffn // block
    width = (2 * heads + 2) * dim
    one = pl.Buffered(1)
    whole = lambda shape: pl.BlockSpec(shape, lambda i: (0,) * len(shape), pipeline_mode=one)
    cols = pl.BlockSpec((model, block), lambda i: (0, jnp.minimum(i, blocks - 1)))
    mine = lambda size: pl.BlockSpec((model, size), lambda i: (0, lax.axis_index('sp')), pipeline_mode=one)
    away = pl.BlockSpec(memory_space=pl.ANY)
    dma = pltpu.SemaphoreType.DMA
    vmem = pltpu.VMEM
    shape = jax.ShapeDtypeStruct
    return pl.pallas_call(
        functools.partial(front_kernel, count=count, blocks=blocks, heads=heads, dim=dim),
        grid=(blocks + batch,),
        in_specs=[whole((rows, model)), whole((rows, model)), cols, cols, pl.BlockSpec((block, model), lambda i: (jnp.minimum(i, blocks - 1), 0)), whole(rope.shape),
                  mine(heads * dim), mine(dim), mine(dim), pl.BlockSpec((heads * dim, model), lambda i: (lax.axis_index('sp'), 0), pipeline_mode=one),
                  whole(q_norm.shape), whole(k_norm.shape)],
        out_specs=[whole((rows, model)), whole((rows, model)), away, away,
                   pl.BlockSpec((count, 1, piece, width), lambda i: (0, jnp.maximum(i - blocks, 0), 0, 0)), whole((8, dim)), whole((model, width // 2)), whole((model, width // 2))],
        out_shape=[shape((rows, model), BF16), shape((rows, model), F32), shape((batch, count, piece, model), BF16), shape((batch, count, piece, model), BF16),
                   shape((count, batch, piece, width), BF16), shape((8, dim), F32), shape((model, width // 2), BF16), shape((model, width // 2), BF16)],
        scratch_shapes=[vmem((batch, count, piece, model), BF16), vmem((batch, count, piece, model), BF16), vmem((count,) + rope.shape, F32), vmem((rows, model), F32),
                        vmem((count * piece, dim), F32), vmem((count * piece, dim), F32), vmem(((heads + 2) * dim, model), F32), vmem((heads * dim, model), F32),
                        dma((batch, 14)), dma((batch, 14)), dma((count - 1,)), dma((count - 1,)), dma((batch, 2))],
        compiler_params=pltpu.CompilerParams(vmem_limit_bytes=62 * 2 ** 20, collective_id=0, has_side_effects=True),
        cost_estimate=pl.CostEstimate(flops=12 * rows * model * ffn + 8 * batch * count * piece * model * width, bytes_accessed=6 * model * ffn, transcendentals=0),
    )(n, dy, w_gate, w_up, w_down, rope, w_q, w_k, w_v, w_o, q_norm, k_norm)


def norm_kernel(x_ref, gain_ref, n_ref):
    x = x_ref[...].astype(F32)
    centered = x - jnp.mean(x, axis=-1, keepdims=True)
    scale = lax.rsqrt(jnp.mean(centered * centered, axis=-1, keepdims=True) + NORM_EPS)
    n_ref[...] = (centered * scale * gain_ref[...]).astype(BF16)


def input_norm(x, gain):
    rows, model = x.shape
    tile = rows // 4
    return pl.pallas_call(
        norm_kernel,
        grid=(rows // tile,),
        in_specs=[pl.BlockSpec((tile, model), lambda i: (i, 0)), pl.BlockSpec((1, model), lambda i: (0, 0))],
        out_specs=pl.BlockSpec((tile, model), lambda i: (i, 0)),
        out_shape=jax.ShapeDtypeStruct((rows, model), BF16),
        cost_estimate=pl.CostEstimate(flops=8 * rows * model, bytes_accessed=4 * rows * model, transcendentals=0),
    )(x, gain)


def finish_kernel(core_ref, mix_ref, x_ref, dy_ref, m_ref, dn_ref, gain_ref, wq_ref, wk_ref, wv_ref, wo_ref, gg_ref, gu_ref, gd_ref, pg_ref, pu_ref, pd_ref, qk_ref, vo_ref,
                  y_ref, dx_ref, gain_grad_ref, fg_ref, fu_ref, fd_ref, fq_ref, fk_ref, fv_ref, fo_ref, a_acc, d_acc, col_buf, row_buf, qk_buf, vo_buf, in_sem, out_sem, *, parts):
    step = pl.program_id(0)
    steps = pl.num_programs(0)
    o_size, k_size = parts
    share = gg_ref.shape[1]
    slots, _, col_rows, _ = col_buf.shape
    row_rows = row_buf.shape[2]
    mine, theirs = pl.multiple_of(core_ref[0] * share, share), pl.multiple_of((1 - core_ref[0]) * share, share)

    def fetches(at):
        slot = lax.rem(at, slots)
        cols = pl.ds(pl.multiple_of(at * col_rows, col_rows), col_rows)
        rows = pl.ds(pl.multiple_of(at * row_rows, row_rows), row_rows)
        pairs = [(ref.at[cols], col_buf.at[slot, i]) for i, ref in enumerate((gg_ref, gu_ref, pg_ref, pu_ref))]
        pairs += [(ref.at[rows], row_buf.at[slot, i]) for i, ref in enumerate((gd_ref, pd_ref))]
        pairs += [(qk_ref.at[at], qk_buf.at[slot]), (vo_ref.at[at], vo_buf.at[slot])]
        return [pltpu.make_async_copy(src, dst, in_sem.at[slot, i]) for i, (src, dst) in enumerate(pairs)]

    def places(at):
        slot = lax.rem(at, slots)
        cols = pl.ds(pl.multiple_of(at * col_rows, col_rows), col_rows)
        pairs = [(col_buf.at[slot, i], ref.at[cols, pl.ds(start, share)]) for i, (ref, start) in enumerate(((fg_ref, mine), (fu_ref, mine), (fg_ref, theirs), (fu_ref, theirs)))]
        pairs += [(row_buf.at[slot, i], fd_ref.at[pl.ds(pl.multiple_of(start + at * row_rows, row_rows), row_rows)]) for i, start in enumerate((mine, theirs))]
        qk, vo = qk_buf.at[slot], vo_buf.at[slot]
        at_o, at_k = pl.ds(pl.multiple_of(at * o_size, o_size), o_size), pl.ds(pl.multiple_of(at * k_size, k_size), k_size)
        pairs += [(qk.at[:, pl.ds(0, o_size)], fq_ref.at[:, at_o]), (qk.at[:, pl.ds(o_size, k_size)], fk_ref.at[:, at_k]), (vo.at[:, pl.ds(0, k_size)], fv_ref.at[:, at_k])]
        pairs += [(vo.at[pl.ds(i * o_size, o_size), pl.ds(k_size, o_size)], fo_ref.at[at_o, pl.ds(i * o_size, o_size)]) for i in range(qk.shape[0] // o_size)]
        return [pltpu.make_async_copy(src, dst, out_sem.at[slot, i]) for i, (src, dst) in enumerate(pairs)]

    @pl.when(step == 0)
    def _():
        for copy in fetches(0):
            copy.start()

    @pl.when(step > 1)
    def _():
        for copy in places(step - 2):
            copy.wait()

    @pl.when(step < steps - 1)
    def _():
        for copy in fetches(step + 1):
            copy.start()

    mix = mix_ref[0]
    a_new = dot_nn(mix[:, :o_size], wo_ref[...])
    d_new = dot_nt(mix[:, o_size:2 * o_size], wq_ref[...])
    d_new += dot_nt(mix[:, 2 * o_size:2 * o_size + k_size], wk_ref[...]) + dot_nt(mix[:, 2 * o_size + k_size:], wv_ref[...])

    @pl.when(step == 0)
    def _():
        a_acc[...] = a_new
        d_acc[...] = d_new + dn_ref[...]

    @pl.when(step > 0)
    def _():
        a_acc[...] += a_new
        d_acc[...] += d_new

    for copy in fetches(step):
        copy.wait()
    for copy in places(step):
        copy.start()

    @pl.when(step == steps - 1)
    def _():
        x = x_ref[...].astype(F32)
        y_ref[...] = (x + a_acc[...].astype(BF16).astype(F32) + m_ref[...].astype(F32)).astype(BF16)
        centered = x - jnp.mean(x, axis=-1, keepdims=True)
        scale = lax.rsqrt(jnp.mean(centered * centered, axis=-1, keepdims=True) + NORM_EPS)
        unit = centered * scale
        grad = d_acc[...].astype(BF16).astype(F32)
        gain_grad = jnp.sum(grad * unit, axis=0, keepdims=True)
        rows, lanes = gain_grad_ref.shape
        for i in range(rows):
            gain_grad_ref[i:i + 1, :] = gain_grad[:, i * lanes:(i + 1) * lanes]
        grad = grad * gain_ref[...]
        along = jnp.mean(grad * unit, axis=-1, keepdims=True)
        grad = scale * (grad - jnp.mean(grad, axis=-1, keepdims=True) - unit * along)
        dx_ref[...] = (dy_ref[...].astype(F32) + grad).astype(BF16)
        for copy in places(step - 1) + places(step):
            copy.wait()


def finish(core, mix, x, dy, mlp_out, d_norm, gain, w_q, w_k, w_v, w_o, own_grads, partner_grads, qk, vo, o_size, k_size):
    rows, model = x.shape
    pieces, _, width = mix.shape
    share = own_grads[0].shape[1]
    whole = pl.BlockSpec((rows, model), lambda i, c: (0, 0))
    row = pl.BlockSpec((1, model), lambda i, c: (0, 0))
    gain_shape = (model // k_size, k_size)
    cols = lambda size: pl.BlockSpec((model, size), lambda i, c: (0, i))
    away = pl.BlockSpec(memory_space=pl.ANY)
    bf16 = lambda *shape: jax.ShapeDtypeStruct(shape, BF16)
    return pl.pallas_call(
        functools.partial(finish_kernel, parts=(o_size, k_size)),
        grid_spec=pltpu.PrefetchScalarGridSpec(
            num_scalar_prefetch=1,
            grid=(pieces,),
            in_specs=[pl.BlockSpec((1, rows, width), lambda i, c: (i, 0, 0))] + [whole] * 4
            + [row, cols(o_size), cols(k_size), cols(k_size), pl.BlockSpec((o_size, model), lambda i, c: (i, 0))] + [away] * 8,
            out_specs=[whole, whole, pl.BlockSpec(gain_shape, lambda i, c: (0, 0))] + [away] * 7,
            scratch_shapes=[pltpu.VMEM((rows, model), F32), pltpu.VMEM((rows, model), F32),
                            pltpu.VMEM((3, 4, model // pieces, share), BF16), pltpu.VMEM((3, 2, share // pieces, model), BF16),
                            pltpu.VMEM((3,) + qk.shape[1:], BF16), pltpu.VMEM((3,) + vo.shape[1:], BF16),
                            pltpu.SemaphoreType.DMA((3, 8)), pltpu.SemaphoreType.DMA((3, 9 + model // o_size))],
        ),
        out_shape=[bf16(rows, model), bf16(rows, model), jax.ShapeDtypeStruct(gain_shape, F32)]
        + [bf16(model, 2 * share), bf16(model, 2 * share), bf16(2 * share, model)] + [bf16(*weight.shape) for weight in (w_q, w_k, w_v, w_o)],
        compiler_params=pltpu.CompilerParams(vmem_limit_bytes=56 * 2 ** 20),
        cost_estimate=pl.CostEstimate(flops=2 * pieces * rows * width * model, bytes_accessed=14 * rows * model + 2 * pieces * width * (rows + model), transcendentals=0),
    )(core, mix, x, dy, mlp_out, d_norm, gain, w_q, w_k, w_v, w_o, *own_grads, *partner_grads, qk, vo)


def share_kernel(gain_ref, norm_ref, gain_out, q_out, k_out, parts, send_sem, recv_sem, *, count, heads):
    me = lax.axis_index('sp')
    rows = gain_ref.shape[0]
    meet(count)
    copies = [pltpu.make_async_remote_copy(src_ref=src, dst_ref=parts.at[me, pl.ds(j * rows, rows)], send_sem=send_sem.at[i, j], recv_sem=recv_sem.at[i, j],
                                           device_id={'sp': device}, device_id_type=MESH)
              for i, device in enumerate(other_devices(count)) for j, src in enumerate((gain_ref, norm_ref))]
    for copy in copies:
        copy.start()
    parts[pl.ds(me, 1), :rows] = gain_ref[...][None]
    parts[pl.ds(me, 1), rows:] = norm_ref[...][None]
    for copy in copies:
        copy.wait()
    gain_out[...] = jnp.sum(parts[:, :rows], axis=0)
    for device in range(count):
        q_out[device * heads:(device + 1) * heads, :] = parts[device, rows:rows + heads, :]
        k_out[device:device + 1, :] = parts[device, rows + heads:rows + heads + 1, :]


def share_small(gain, norms, q_norm, k_norm, count):
    vmem = pl.BlockSpec(memory_space=pltpu.VMEM)
    heads = q_norm.shape[0] // k_norm.shape[0]
    dma = pltpu.SemaphoreType.DMA((count - 1, 2))
    return pl.pallas_call(
        functools.partial(share_kernel, count=count, heads=heads),
        in_specs=[vmem] * 2,
        out_specs=[vmem] * 3,
        out_shape=[jax.ShapeDtypeStruct(part.shape, F32) for part in (gain, q_norm, k_norm)],
        scratch_shapes=[pltpu.VMEM((count, 2 * gain.shape[0], gain.shape[1]), F32), dma, dma],
        compiler_params=pltpu.CompilerParams(collective_id=2, has_side_effects=True),
    )(gain, norms)


def solution(mesh):
    n_sp = mesh.shape['sp']
    seq_spec = P('dp', 'sp', None)
    grad_spec = P('dp', None)

    def layer_step(x_in, grad_y, positions, w_q, w_k, w_v, w_o, w_gate, w_up, w_down, norm_gain, q_norm, k_norm):
        batch, piece, model = x_in.shape
        num_heads, dim = q_norm.shape
        heads = num_heads // k_norm.shape[0]
        ffn = w_gate.shape[1]
        tokens = batch * piece
        me = lax.axis_index('sp')
        gain_row = norm_gain.reshape(1, model)
        x_rows, dy_own = x_in.reshape(tokens, model), grad_y.reshape(tokens, model)
        n_own = input_norm(x_rows, gain_row)

        inv_freq = ROPE_THETA ** (-(jnp.arange(dim // 2, dtype=F32) * 2.0) / dim)
        angles = jnp.repeat(positions.astype(F32)[:, None] * inv_freq[None, :], 2, axis=1)
        sign = jnp.where(jnp.arange(dim) % 2 == 0, -1.0, 1.0).astype(F32)
        rope_own = jnp.stack([jnp.cos(angles), jnp.sin(angles) * sign[None, :]])

        mlp_out, d_norm, n_all, dy_all, mix, norm_grads, qk, vo = front(n_own, dy_own, w_gate, w_up, w_down, rope_own, w_q, w_k, w_v, w_o, q_norm, k_norm,
                                                                        n_sp, piece, ffn // 6)
        by_tile = lambda part: part.reshape(n_sp, -1, part.shape[-1])
        *grads, mix, qk, vo = all_mlp(by_tile(n_all), by_tile(dy_all), w_gate, w_up, w_down, by_tile(mix), qk, vo, ffn // 6)

        y_out, grad_x, grad_gain, full_gate, full_up, full_down, full_q, full_k, full_v, full_o = finish(
            (me % 2).reshape(1), mix, x_rows, dy_own, mlp_out, d_norm, gain_row, w_q, w_k, w_v, w_o, grads[:3], grads[3:], qk, vo, heads * dim, dim)
        full_gain, full_qn, full_kn = share_small(grad_gain, norm_grads, q_norm, k_norm, n_sp)
        return (y_out.reshape(x_in.shape), grad_x.reshape(x_in.shape), full_q, full_k, full_v, full_o, full_gate, full_up, full_down,
                full_gain.reshape(model), full_qn, full_kn)

    in_specs = (seq_spec, seq_spec, P(('dp', 'sp'))) + (P(),) * 10
    out_specs = (seq_spec, seq_spec) + (grad_spec,) * 7 + (P('dp'), grad_spec, grad_spec)
    return jax.shard_map(layer_step, mesh=mesh, in_specs=in_specs, out_specs=out_specs, check_vma=False)
```

```python
import functools

import jax
import jax.numpy as jnp
from jax import lax
from jax.experimental import pallas as pl
from jax.experimental.pallas import tpu as pltpu
from jax.sharding import PartitionSpec as P

NORM_EPS = 1e-5
ROPE_THETA = 75.0e6
F32 = jnp.float32
BF16 = jnp.bfloat16
MESH = pl.DeviceIdType.MESH


def dot_nn(lhs, rhs):
    return lax.dot_general(lhs, rhs, (((1,), (0,)), ((), ())), preferred_element_type=F32)


def dot_nt(lhs, rhs):
    return lax.dot_general(lhs, rhs, (((1,), (1,)), ((), ())), preferred_element_type=F32)


def swiglu_both(gate, up, d_hidden):
    sig = jax.nn.sigmoid(gate)
    act = gate * sig
    d_hidden = d_hidden.astype(BF16).astype(F32)
    d_gate = d_hidden * up * (sig * (1.0 + gate * (1.0 - sig)))
    return (act * up).astype(BF16), d_gate.astype(BF16), (d_hidden * act).astype(BF16)


def other_devices(count):
    me = lax.axis_index('sp')
    return [lax.rem(me + shift, count) for shift in range(1, count)]


def meet(count):
    barrier = pltpu.get_barrier_semaphore()
    for device in other_devices(count):
        pl.semaphore_signal(barrier, inc=1, device_id={'sp': device}, device_id_type=MESH)
    pl.semaphore_wait(barrier, count - 1)


def all_mlp_kernel(n_ref, dy_ref, wg_ref, wu_ref, wd_ref, mix_ref, qk_ref, vo_ref, gg_ref, gu_ref, gd_ref, pg_ref, pu_ref, pd_ref, swap_ref, qk_all, vo_all,
                   n_t, dy_t, acc_g, acc_u, acc_d, swap_send, swap_recv, half_send, half_recv, ring_send, ring_recv, own_sem, *, block, count):
    step = pl.program_id(0)
    last = pl.num_programs(0) - 1
    share = wg_ref.shape[1]
    me = lax.axis_index('sp')
    right, left, across, partner = lax.rem(me + 2, count), lax.rem(me + count - 2, count), lax.rem(me + 4, count), me + 1 - 2 * lax.rem(me, 2)
    other = lambda device: device + 1 - 2 * lax.rem(device, 2)

    tail = pl.ds(mix_ref.shape[1] - swap_ref.shape[1], swap_ref.shape[1])

    def swaps(shifts):
        copies = []
        for shift in shifts:
            device = lax.rem(me + shift, count)
            copies.append(pltpu.make_async_remote_copy(src_ref=mix_ref.at[device, tail], dst_ref=swap_ref.at[me], send_sem=swap_send.at[shift - 1], recv_sem=swap_recv.at[shift - 1],
                                                       device_id={'sp': device}, device_id_type=MESH))
        return copies

    def halves(i):
        cols = pl.ds(i * block, block)
        return [pltpu.make_async_remote_copy(src_ref=src.at[index], dst_ref=dst.at[index], send_sem=half_send.at[i, j], recv_sem=half_recv.at[i, j],
                                             device_id={'sp': partner}, device_id_type=MESH)
                for j, (src, dst, index) in enumerate(((gg_ref, pg_ref, (slice(None), cols)), (gu_ref, pu_ref, (slice(None), cols)), (gd_ref, pd_ref, (cols,))))]

    def send(index, src, into, slot, target):
        return pltpu.make_async_remote_copy(src_ref=src, dst_ref=into.at[slot], send_sem=ring_send.at[index], recv_sem=ring_recv.at[index],
                                            device_id={'sp': target}, device_id_type=MESH)

    def forward(index, ref, slot, target):
        return send(index, ref.at[slot], ref, slot, target)

    def arrived(index, ref, slot):
        send(index, ref.at[slot], ref, slot, partner).wait_recv()

    own = lambda: [send(0, vo_ref, vo_all, me, right), send(2, qk_ref, qk_all, me, left), send(1, qk_ref, qk_all, me, right),
                   send(3, vo_ref, vo_all, me, left), send(4, qk_ref, qk_all, me, partner), send(5, vo_ref, vo_all, me, partner)]
    early = lambda: [forward(6, vo_all, left, right), forward(7, qk_all, right, left), forward(8, vo_all, left, partner), forward(9, qk_all, right, partner)]
    late = lambda: [forward(10, qk_all, left, partner), forward(11, vo_all, right, partner), forward(12, vo_all, across, partner), forward(13, qk_all, across, partner)]
    keep = lambda: [pltpu.make_async_copy(mix_ref.at[me, tail], swap_ref.at[me], own_sem.at[0]), pltpu.make_async_copy(qk_ref, qk_all.at[me], own_sem.at[1]),
                    pltpu.make_async_copy(vo_ref, vo_all.at[me], own_sem.at[2])]

    @pl.when(step == 0)
    def _():
        meet(count)
        for copy in own() + swaps((1, count - 1, 2, count - 2)) + keep():
            copy.start()
        acc_g[...] = jnp.zeros_like(acc_g)
        acc_u[...] = jnp.zeros_like(acc_u)
        acc_d[...] = jnp.zeros_like(acc_d)

    @pl.when(step == 2)
    def _():
        arrived(0, vo_all, left)
        arrived(2, qk_all, right)
        for copy in early() + swaps(range(3, count - 2)):
            copy.start()

    def pass_late(parts):
        copies = late()
        for i in parts:
            index, ref, slot = ((1, qk_all, left), (3, vo_all, right), (6, vo_all, across), (7, qk_all, across))[i]
            arrived(index, ref, slot)
            copies[i].start()

    @pl.when(step == last - 1)
    def _():
        pass_late((0, 1))

    n_t[...] = n_ref[0].T
    dy_t[...] = dy_ref[0].T

    @pl.loop(0, share // block)
    def _(i):
        cols = pl.ds(pl.multiple_of(i * block, block), block)
        n, dy = n_ref[0], dy_ref[0]
        hidden, d_gate, d_up = swiglu_both(dot_nn(n, wg_ref[:, cols]), dot_nn(n, wu_ref[:, cols]), dot_nt(dy, wd_ref[cols, :]))
        acc_g[:, cols] += dot_nn(n_t[...], d_gate)
        acc_u[:, cols] += dot_nn(n_t[...], d_up)
        acc_d[:, cols] += dot_nn(dy_t[...], hidden)

        @pl.when(step == last)
        def _():
            gg_ref[:, cols] = acc_g[:, cols].astype(BF16)
            gu_ref[:, cols] = acc_u[:, cols].astype(BF16)
            gd_ref[cols, :] = acc_d[:, cols].T.astype(BF16)

        for done in range(share // block - 1):
            @pl.when((step == last) & (i == done + 1))
            def _():
                for copy in halves(done):
                    copy.start()

    @pl.when(step == last)
    def _():
        for copy in halves(share // block - 1):
            copy.start()
        pass_late((2, 3))
        for index, ref, slot in ((4, qk_all, partner), (5, vo_all, partner), (8, vo_all, other(left)), (9, qk_all, other(right)),
                                 (10, qk_all, other(left)), (11, vo_all, other(right)), (12, vo_all, other(across)), (13, qk_all, other(across))):
            arrived(index, ref, slot)
        for copy in own() + early() + late():
            copy.wait_send()
        for copy in swaps(range(1, count)):
            copy.wait()
        for copy in keep():
            copy.wait()
        for i in range(share // block):
            for copy in halves(i):
                copy.wait()


def all_mlp(n, dy, w_gate, w_up, w_down, mix, lead, qk, vo, block):
    count, tile, model = n.shape
    share = w_gate.shape[1] // 2
    tok = pl.BlockSpec((1, tile, model), lambda i: (i, 0, 0))
    one = pl.Buffered(1)
    core = lambda: lax.rem(lax.axis_index('sp'), 2)
    in_cols = pl.BlockSpec((model, share), lambda i: (0, core()), pipeline_mode=one)
    out_cols = pl.BlockSpec((model, share), lambda i: (0, 0), pipeline_mode=one)
    away = pl.BlockSpec(memory_space=pl.ANY)
    dma = pltpu.SemaphoreType.DMA
    shape = lambda *dims: jax.ShapeDtypeStruct(dims, BF16)
    grads = [shape(model, share), shape(model, share), shape(share, model)]
    return pl.pallas_call(
        functools.partial(all_mlp_kernel, block=block, count=count),
        grid=(count,),
        in_specs=[tok, tok, in_cols, in_cols, pl.BlockSpec((share, model), lambda i: (core(), 0), pipeline_mode=one), away, away, away],
        out_specs=[out_cols, out_cols, pl.BlockSpec((share, model), lambda i: (0, 0), pipeline_mode=one)] + [away] * 6,
        out_shape=grads + grads + [shape(count, mix.shape[1] - lead, *mix.shape[2:]), shape(count, *qk.shape), shape(count, *vo.shape)],
        scratch_shapes=[pltpu.VMEM((model, tile), BF16)] * 2 + [pltpu.VMEM((model, share), F32)] * 3
        + [dma((count - 1,)), dma((count - 1,)), dma((share // block, 3)), dma((share // block, 3)), dma((14,)), dma((14,)), dma((3,))],
        compiler_params=pltpu.CompilerParams(vmem_limit_bytes=61 * 2 ** 20, collective_id=1, has_side_effects=True),
        cost_estimate=pl.CostEstimate(flops=12 * count * tile * model * share, bytes_accessed=4 * model * count * tile + 12 * model * share, transcendentals=0),
    )(n, dy, w_gate, w_up, w_down, mix, qk, vo)


def swap_pairs(rows):
    width = rows.shape[1]
    lane = lax.broadcasted_iota(jnp.int32, rows.shape, 1)
    return jnp.where(lane % 2 == 0, pltpu.roll(rows, width - 1, 1), pltpu.roll(rows, 1, 1))


def head_forward(rows, weight, cos_t, sin_t):
    rows = rows.astype(F32)
    centered = rows - jnp.mean(rows, axis=-1, keepdims=True)
    scale = lax.rsqrt(jnp.mean(centered * centered, axis=-1, keepdims=True) + NORM_EPS)
    unit = centered * scale
    normed = unit * weight
    return (normed * cos_t + swap_pairs(normed) * sin_t).astype(BF16), unit, scale


def head_backward(grad, unit, scale, weight, cos_t, sin_t):
    grad = grad.astype(BF16).astype(F32)
    grad = grad * cos_t - swap_pairs(grad) * sin_t
    weight_grad = jnp.sum(grad * unit, axis=0, keepdims=True)
    grad = grad * weight
    along = jnp.mean(grad * unit, axis=-1, keepdims=True)
    grad = scale * (grad - jnp.mean(grad, axis=-1, keepdims=True) - unit * along)
    return grad.astype(BF16), weight_grad


def one_sequence(me, n_rows, dy_rows, cos_t, sin_t, wq_ref, wk_ref, wv_ref, wo_ref, qn_ref, kn_ref, mix_ref, wn_ref, k_acc, v_acc, qkv_acc, o_acc, heads, dim, block):
    pieces, _, piece, _ = mix_ref.shape
    full = pieces * piece
    score_scale = dim ** -0.5
    width = heads * dim

    def put(start, rows):
        mix_ref[:, 0, :, start:start + rows.shape[1]] = rows.reshape(pieces, piece, rows.shape[1])

    q_proj = dot_nn(n_rows, wq_ref[...]).astype(BF16)
    k_proj = dot_nn(n_rows, wk_ref[...]).astype(BF16)
    v_rows = dot_nn(n_rows, wv_ref[...]).astype(BF16)
    d_out = dot_nt(dy_rows, wo_ref[...]).astype(BF16)
    q_weights = [qn_ref[pl.ds(me * heads + h, 1), :] for h in range(heads)]
    k_weight = kn_ref[pl.ds(me, 1), :]
    q_parts = [head_forward(q_proj[:, h * dim:(h + 1) * dim], q_weights[h], cos_t, sin_t) for h in range(heads)]
    k_rot, k_unit, k_scale = head_forward(k_proj, k_weight, cos_t, sin_t)
    k_t, v_t = k_rot.T, v_rows.T
    o_blocks, dq_blocks = [[] for _ in range(heads)], [[] for _ in range(heads)]
    for start in range(full - block, -1, -block):
        stop = start + block
        q_blk = jnp.concatenate([q_parts[h][0][start:stop] for h in range(heads)], axis=0)
        do_blk = jnp.concatenate([d_out[start:stop, h * dim:(h + 1) * dim] for h in range(heads)], axis=0)
        k_blk, v_blk = k_rot[:stop], v_rows[:stop]
        scores = dot_nt(k_blk, q_blk)
        tail = scores[start:]
        key = lax.broadcasted_iota(jnp.int32, tail.shape, 0)
        query = lax.broadcasted_iota(jnp.int32, tail.shape, 1) % block
        tail = jnp.where(query >= key, tail, -1e30)
        scores = tail if start == 0 else jnp.concatenate([scores[:start], tail], axis=0)
        top = jnp.max(scores, axis=0, keepdims=True)
        probs = jnp.exp((scores - top) * score_scale)
        probs = probs * (1.0 / jnp.sum(probs, axis=0, keepdims=True))
        probs_b = probs.astype(BF16)
        o_blk = dot_nn(v_t[:, :stop], probs_b).astype(BF16)
        d_probs = dot_nt(v_blk, do_blk)
        delta = jnp.sum(probs * d_probs, axis=0, keepdims=True)
        d_scores = (probs * (d_probs - delta)).astype(BF16)
        dq_blk = dot_nn(k_t[:, :stop], d_scores) * score_scale
        dk_new, dv_new = dot_nn(d_scores, q_blk), dot_nn(probs_b, do_blk)
        if stop == full:
            k_acc[...], v_acc[...] = dk_new, dv_new
        else:
            k_acc[0:stop, :] += dk_new
            v_acc[0:stop, :] += dv_new
        for h in range(heads):
            o_blocks[h].append(o_blk[:, h * block:(h + 1) * block])
            dq_blocks[h].append(dq_blk[:, h * block:(h + 1) * block].T)
    for h in range(heads):
        o_t = jnp.concatenate(o_blocks[h][::-1], axis=1)
        put(h * dim, o_t.T)
        o_acc[h * dim:(h + 1) * dim, :] += dot_nn(o_t, dy_rows)
        _, unit, scale = q_parts[h]
        dq, weight_grad = head_backward(jnp.concatenate(dq_blocks[h][::-1], axis=0), unit, scale, q_weights[h], cos_t, sin_t)
        put(width + h * dim, dq)
        qkv_acc[h * dim:(h + 1) * dim, :] += dot_nn(dq.T, n_rows)
        wn_ref[h:h + 1, :] += weight_grad
    dk, weight_grad = head_backward(k_acc[...] * score_scale, k_unit, k_scale, k_weight, cos_t, sin_t)
    wn_ref[heads:heads + 1, :] += weight_grad
    dv = v_acc[...].astype(BF16)
    put(2 * width, dk)
    put(2 * width + dim, dv)
    qkv_acc[width:width + dim, :] += dot_nn(dk.T, n_rows)
    qkv_acc[width + dim:width + 2 * dim, :] += dot_nn(dv.T, n_rows)


def front_kernel(n_ref, dy_ref, wg_ref, wu_ref, wd_ref, rope_ref, wq_ref, wk_ref, wv_ref, wo_ref, qn_ref, kn_ref,
                 m_ref, dn_ref, gn_ref, gdy_ref, mix_ref, lead_ref, wn_ref, qk_ref, vo_ref,
                 mix_buf, n_all, dy_all, rope_all, m_acc, k_acc, v_acc, qkv_acc, o_acc, send_sem, recv_sem, rope_send, rope_recv, out_sem, mix_sem, lead_send, lead_recv, lead_sem, *, count, blocks, heads, dim):
    step = pl.program_id(0)
    me = lax.axis_index('sp')
    right, left, across, partner = lax.rem(me + 2, count), lax.rem(me + count - 2, count), lax.rem(me + 4, count), me + 1 - 2 * lax.rem(me, 2)
    other = lambda device: device + 1 - 2 * lax.rem(device, 2)
    batch, _, piece, model = n_all.shape

    def send(seq, index, src, into, slot, target):
        return pltpu.make_async_remote_copy(src_ref=src, dst_ref=into.at[seq, slot], send_sem=send_sem.at[seq, index], recv_sem=recv_sem.at[seq, index],
                                            device_id={'sp': target}, device_id_type=MESH)

    def forward(seq, index, ref, slot, target):
        return send(seq, index, ref.at[seq, slot], ref, slot, target)

    def own(seq):
        rows = pl.ds(pl.multiple_of(seq * piece, piece), piece)
        n, dy = n_ref.at[rows], dy_ref.at[rows]
        return [send(seq, 0, dy, dy_all, me, right), send(seq, 2, n, n_all, me, left), send(seq, 1, n, n_all, me, right),
                send(seq, 3, dy, dy_all, me, left), send(seq, 4, n, n_all, me, partner), send(seq, 5, dy, dy_all, me, partner)]

    def early(seq):
        return [forward(seq, 6, dy_all, left, right), forward(seq, 8, dy_all, left, partner), forward(seq, 7, n_all, right, left), forward(seq, 9, n_all, right, partner)]

    def late(seq):
        return [forward(seq, 10, n_all, left, partner), forward(seq, 11, dy_all, right, partner),
                forward(seq, 12, dy_all, across, partner), forward(seq, 13, n_all, across, partner)]

    def arrived(seq, index, ref, slot):
        send(seq, index, ref.at[seq, slot], ref, slot, partner).wait_recv()

    def start_own(seq):
        for copy in own(seq):
            copy.start()

    def pass_early(seq):
        copies = early(seq)
        arrived(seq, 0, dy_all, left)
        copies[0].start()
        copies[1].start()
        arrived(seq, 2, n_all, right)
        copies[2].start()
        copies[3].start()

    def pass_late(seq):
        for copy, (index, ref, slot) in zip(late(seq), ((1, n_all, left), (3, dy_all, right), (6, dy_all, across), (7, n_all, across))):
            arrived(seq, index, ref, slot)
            copy.start()

    def complete(seq):
        for index, ref, slot in ((4, n_all, partner), (5, dy_all, partner), (8, dy_all, other(left)), (9, n_all, other(right)),
                                 (10, n_all, other(left)), (11, dy_all, other(right)), (12, dy_all, other(across)), (13, n_all, other(across))):
            arrived(seq, index, ref, slot)

    def tables():
        return [pltpu.make_async_remote_copy(src_ref=rope_ref, dst_ref=rope_all.at[me], send_sem=rope_send.at[i], recv_sem=rope_recv.at[i],
                                             device_id={'sp': device}, device_id_type=MESH) for i, device in enumerate(other_devices(count))]

    def to_memory(seq):
        return [pltpu.make_async_copy(n_all.at[seq], gn_ref.at[seq], out_sem.at[seq, 0]), pltpu.make_async_copy(dy_all.at[seq], gdy_ref.at[seq], out_sem.at[seq, 1])]

    def mix_out(seq):
        return pltpu.make_async_copy(mix_buf.at[lax.rem(seq, 2), :, 0], mix_ref.at[:, seq], mix_sem.at[lax.rem(seq, 2)])

    def lead_swaps():
        ahead = pl.ds(0, lead_ref.shape[1])
        return [pltpu.make_async_copy(mix_ref.at[me, ahead], lead_ref.at[me], lead_sem)] + [
            pltpu.make_async_remote_copy(src_ref=mix_ref.at[device, ahead], dst_ref=lead_ref.at[me], send_sem=lead_send.at[i], recv_sem=lead_recv.at[i],
                                         device_id={'sp': device}, device_id_type=MESH) for i, device in enumerate(other_devices(count))]

    @pl.when(step == 0)
    def _():
        meet(count)
        start_own(0)
        for copy in tables():
            copy.start()
        start_own(1)
        for seq in range(batch):
            rows = slice(seq * piece, (seq + 1) * piece)
            n_all[seq, pl.ds(me, 1)] = n_ref[rows, :][None]
            dy_all[seq, pl.ds(me, 1)] = dy_ref[rows, :][None]
        rope_all[pl.ds(me, 1)] = rope_ref[...][None]
        wn_ref[...] = jnp.zeros_like(wn_ref)
        qkv_acc[...] = jnp.zeros_like(qkv_acc)
        o_acc[...] = jnp.zeros_like(o_acc)

    @pl.when(step == 2)
    def _():
        pass_early(0)
        start_own(2)

    @pl.when(step == blocks - 2)
    def _():
        pass_early(1)
        start_own(3)

    @pl.when(step == blocks - 1)
    def _():
        pass_late(0)

    @pl.when(step < blocks)
    def _():
        n, dy = n_ref[...], dy_ref[...]
        wg, wu, wd = wg_ref[...], wu_ref[...], wd_ref[...]
        hidden, d_gate, d_up = swiglu_both(dot_nn(n, wg), dot_nn(n, wu), dot_nt(dy, wd))
        m_new = dot_nn(hidden, wd)
        dn_new = dot_nt(d_gate, wg) + dot_nt(d_up, wu)

        @pl.when(step == 0)
        def _():
            m_acc[...] = m_new
            dn_ref[...] = dn_new

        @pl.when(step > 0)
        def _():
            m_acc[...] += m_new
            dn_ref[...] += dn_new

        @pl.when(step == blocks - 1)
        def _():
            m_ref[...] = m_acc[...].astype(BF16)

    @pl.when(step == blocks)
    def _():
        for copy in tables():
            copy.wait()

    @pl.when(step >= blocks)
    def _():
        seq = step - blocks

        @pl.when(seq + 2 < batch)
        def _():
            pass_early(seq + 2)

        @pl.when(seq + 4 < batch)
        def _():
            start_own(seq + 4)

        @pl.when(seq + 1 < batch)
        def _():
            pass_late(seq + 1)

        @pl.when(seq > 1)
        def _():
            mix_out(seq - 2).wait()

        @pl.when(seq == batch - 3)
        def _():
            for copy in lead_swaps():
                copy.start()

        complete(seq)
        for copy in to_memory(seq):
            copy.start()
        full = count * piece
        one_sequence(me, n_all[seq].reshape(full, model), dy_all[seq].reshape(full, model), rope_all[:, 0].reshape(full, dim), rope_all[:, 1].reshape(full, dim),
                     wq_ref, wk_ref, wv_ref, wo_ref, qn_ref, kn_ref, mix_buf.at[lax.rem(seq, 2)], wn_ref, k_acc, v_acc, qkv_acc, o_acc, heads, dim, min(128, full))
        mix_out(seq).start()

    @pl.when(step == pl.num_programs(0) - 1)
    def _():
        size = o_acc.shape[0]
        qk_size = size + dim
        qk_ref[...] = qkv_acc[:qk_size, :].T.astype(BF16)
        vo_ref[:, :dim] = qkv_acc[qk_size:, :].T.astype(BF16)
        for i in range(model // size):
            vo_ref[i * size:(i + 1) * size, dim:] = o_acc[:, i * size:(i + 1) * size].astype(BF16)

        mix_out(batch - 2).wait()
        mix_out(batch - 1).wait()
        for copy in lead_swaps():
            copy.wait()

        @pl.loop(0, batch)
        def _(seq):
            for copy in own(seq) + early(seq) + late(seq):
                copy.wait_send()
            for copy in to_memory(seq):
                copy.wait()


def front(n, dy, w_gate, w_up, w_down, rope, w_q, w_k, w_v, w_o, q_norm, k_norm, count, piece, lead, block):
    rows, model = n.shape
    ffn = w_gate.shape[1]
    num_heads, dim = q_norm.shape
    heads = num_heads // k_norm.shape[0]
    batch = rows // piece
    blocks = ffn // block
    width = (2 * heads + 2) * dim
    one = pl.Buffered(1)
    whole = lambda shape: pl.BlockSpec(shape, lambda i: (0,) * len(shape), pipeline_mode=one)
    cols = pl.BlockSpec((model, block), lambda i: (0, jnp.minimum(i, blocks - 1)))
    mine = lambda size: pl.BlockSpec((model, size), lambda i: (0, lax.axis_index('sp')), pipeline_mode=one)
    away = pl.BlockSpec(memory_space=pl.ANY)
    dma = pltpu.SemaphoreType.DMA
    vmem = pltpu.VMEM
    shape = jax.ShapeDtypeStruct
    return pl.pallas_call(
        functools.partial(front_kernel, count=count, blocks=blocks, heads=heads, dim=dim),
        grid=(blocks + batch,),
        in_specs=[whole((rows, model)), whole((rows, model)), cols, cols, pl.BlockSpec((block, model), lambda i: (jnp.minimum(i, blocks - 1), 0)), whole(rope.shape),
                  mine(heads * dim), mine(dim), mine(dim), pl.BlockSpec((heads * dim, model), lambda i: (lax.axis_index('sp'), 0), pipeline_mode=one),
                  whole(q_norm.shape), whole(k_norm.shape)],
        out_specs=[whole((rows, model)), whole((rows, model)), away, away, away, away, whole((8, dim)), whole((model, width // 2)), whole((model, width // 2))],
        out_shape=[shape((rows, model), BF16), shape((rows, model), F32), shape((batch, count, piece, model), BF16), shape((batch, count, piece, model), BF16),
                   shape((count, batch, piece, width), BF16), shape((count, lead, piece, width), BF16), shape((8, dim), F32), shape((model, width // 2), BF16), shape((model, width // 2), BF16)],
        scratch_shapes=[vmem((2, count, 1, piece, width), BF16), vmem((batch, count, piece, model), BF16), vmem((batch, count, piece, model), BF16), vmem((count,) + rope.shape, F32), vmem((rows, model), F32),
                        vmem((count * piece, dim), F32), vmem((count * piece, dim), F32), vmem(((heads + 2) * dim, model), F32), vmem((heads * dim, model), F32),
                        dma((batch, 14)), dma((batch, 14)), dma((count - 1,)), dma((count - 1,)), dma((batch, 2)), dma((2,)), dma((count - 1,)), dma((count - 1,)), dma],
        compiler_params=pltpu.CompilerParams(vmem_limit_bytes=62 * 2 ** 20, collective_id=0, has_side_effects=True),
        cost_estimate=pl.CostEstimate(flops=12 * rows * model * ffn + 8 * batch * count * piece * model * width, bytes_accessed=6 * model * ffn, transcendentals=0),
    )(n, dy, w_gate, w_up, w_down, rope, w_q, w_k, w_v, w_o, q_norm, k_norm)


def norm_kernel(x_ref, gain_ref, n_ref):
    x = x_ref[...].astype(F32)
    centered = x - jnp.mean(x, axis=-1, keepdims=True)
    scale = lax.rsqrt(jnp.mean(centered * centered, axis=-1, keepdims=True) + NORM_EPS)
    n_ref[...] = (centered * scale * gain_ref[...]).astype(BF16)


def input_norm(x, gain):
    rows, model = x.shape
    tile = rows // 4
    return pl.pallas_call(
        norm_kernel,
        grid=(rows // tile,),
        in_specs=[pl.BlockSpec((tile, model), lambda i: (i, 0)), pl.BlockSpec((1, model), lambda i: (0, 0))],
        out_specs=pl.BlockSpec((tile, model), lambda i: (i, 0)),
        out_shape=jax.ShapeDtypeStruct((rows, model), BF16),
        cost_estimate=pl.CostEstimate(flops=8 * rows * model, bytes_accessed=4 * rows * model, transcendentals=0),
    )(x, gain)


def finish_kernel(core_ref, lead_ref, rest_ref, x_ref, dy_ref, m_ref, dn_ref, gain_ref, wq_ref, wk_ref, wv_ref, wo_ref, gg_ref, gu_ref, gd_ref, pg_ref, pu_ref, pd_ref, qk_ref, vo_ref,
                  y_ref, dx_ref, gain_grad_ref, fg_ref, fu_ref, fd_ref, fq_ref, fk_ref, fv_ref, fo_ref, mix, a_acc, d_acc, col_buf, row_buf, qk_buf, vo_buf, in_sem, out_sem, *, parts):
    step = pl.program_id(0)
    steps = pl.num_programs(0)
    o_size, k_size = parts
    share = gg_ref.shape[1]
    slots, _, col_rows, _ = col_buf.shape
    row_rows = row_buf.shape[2]
    mine, theirs = pl.multiple_of(core_ref[0] * share, share), pl.multiple_of((1 - core_ref[0]) * share, share)

    def fetches(at):
        slot = lax.rem(at, slots)
        cols = pl.ds(pl.multiple_of(at * col_rows, col_rows), col_rows)
        rows = pl.ds(pl.multiple_of(at * row_rows, row_rows), row_rows)
        pairs = [(ref.at[cols], col_buf.at[slot, i]) for i, ref in enumerate((gg_ref, gu_ref, pg_ref, pu_ref))]
        pairs += [(ref.at[rows], row_buf.at[slot, i]) for i, ref in enumerate((gd_ref, pd_ref))]
        pairs += [(qk_ref.at[at], qk_buf.at[slot]), (vo_ref.at[at], vo_buf.at[slot])]
        return [pltpu.make_async_copy(src, dst, in_sem.at[slot, i]) for i, (src, dst) in enumerate(pairs)]

    def places(at):
        slot = lax.rem(at, slots)
        cols = pl.ds(pl.multiple_of(at * col_rows, col_rows), col_rows)
        pairs = [(col_buf.at[slot, i], ref.at[cols, pl.ds(start, share)]) for i, (ref, start) in enumerate(((fg_ref, mine), (fu_ref, mine), (fg_ref, theirs), (fu_ref, theirs)))]
        pairs += [(row_buf.at[slot, i], fd_ref.at[pl.ds(pl.multiple_of(start + at * row_rows, row_rows), row_rows)]) for i, start in enumerate((mine, theirs))]
        qk, vo = qk_buf.at[slot], vo_buf.at[slot]
        at_o, at_k = pl.ds(pl.multiple_of(at * o_size, o_size), o_size), pl.ds(pl.multiple_of(at * k_size, k_size), k_size)
        pairs += [(qk.at[:, pl.ds(0, o_size)], fq_ref.at[:, at_o]), (qk.at[:, pl.ds(o_size, k_size)], fk_ref.at[:, at_k]), (vo.at[:, pl.ds(0, k_size)], fv_ref.at[:, at_k])]
        pairs += [(vo.at[pl.ds(i * o_size, o_size), pl.ds(k_size, o_size)], fo_ref.at[at_o, pl.ds(i * o_size, o_size)]) for i in range(qk.shape[0] // o_size)]
        return [pltpu.make_async_copy(src, dst, out_sem.at[slot, i]) for i, (src, dst) in enumerate(pairs)]

    @pl.when(step == 0)
    def _():
        for copy in fetches(0):
            copy.start()

    @pl.when(step > 1)
    def _():
        for copy in places(step - 2):
            copy.wait()

    @pl.when(step < steps - 1)
    def _():
        for copy in fetches(step + 1):
            copy.start()

    lead = lead_ref.shape[1]
    mix[:lead, :] = lead_ref[0]
    mix[lead:, :] = rest_ref[0]
    a_new = dot_nn(mix[:, :o_size], wo_ref[...])
    d_new = dot_nt(mix[:, o_size:2 * o_size], wq_ref[...])
    d_new += dot_nt(mix[:, 2 * o_size:2 * o_size + k_size], wk_ref[...]) + dot_nt(mix[:, 2 * o_size + k_size:], wv_ref[...])

    @pl.when(step == 0)
    def _():
        a_acc[...] = a_new
        d_acc[...] = d_new + dn_ref[...]

    @pl.when(step > 0)
    def _():
        a_acc[...] += a_new
        d_acc[...] += d_new

    for copy in fetches(step):
        copy.wait()
    for copy in places(step):
        copy.start()

    @pl.when(step == steps - 1)
    def _():
        x = x_ref[...].astype(F32)
        y_ref[...] = (x + a_acc[...].astype(BF16).astype(F32) + m_ref[...].astype(F32)).astype(BF16)
        centered = x - jnp.mean(x, axis=-1, keepdims=True)
        scale = lax.rsqrt(jnp.mean(centered * centered, axis=-1, keepdims=True) + NORM_EPS)
        unit = centered * scale
        grad = d_acc[...].astype(BF16).astype(F32)
        gain_grad = jnp.sum(grad * unit, axis=0, keepdims=True)
        rows, lanes = gain_grad_ref.shape
        for i in range(rows):
            gain_grad_ref[i:i + 1, :] = gain_grad[:, i * lanes:(i + 1) * lanes]
        grad = grad * gain_ref[...]
        along = jnp.mean(grad * unit, axis=-1, keepdims=True)
        grad = scale * (grad - jnp.mean(grad, axis=-1, keepdims=True) - unit * along)
        dx_ref[...] = (dy_ref[...].astype(F32) + grad).astype(BF16)
        for copy in places(step - 1) + places(step):
            copy.wait()


def finish(core, lead, rest, x, dy, mlp_out, d_norm, gain, w_q, w_k, w_v, w_o, own_grads, partner_grads, qk, vo, o_size, k_size):
    rows, model = x.shape
    pieces, _, width = lead.shape
    share = own_grads[0].shape[1]
    whole = pl.BlockSpec((rows, model), lambda i, c: (0, 0))
    row = pl.BlockSpec((1, model), lambda i, c: (0, 0))
    gain_shape = (model // k_size, k_size)
    cols = lambda size: pl.BlockSpec((model, size), lambda i, c: (0, i))
    away = pl.BlockSpec(memory_space=pl.ANY)
    bf16 = lambda *shape: jax.ShapeDtypeStruct(shape, BF16)
    return pl.pallas_call(
        functools.partial(finish_kernel, parts=(o_size, k_size)),
        grid_spec=pltpu.PrefetchScalarGridSpec(
            num_scalar_prefetch=1,
            grid=(pieces,),
            in_specs=[pl.BlockSpec((1, part.shape[1], width), lambda i, c: (i, 0, 0)) for part in (lead, rest)] + [whole] * 4
            + [row, cols(o_size), cols(k_size), cols(k_size), pl.BlockSpec((o_size, model), lambda i, c: (i, 0))] + [away] * 8,
            out_specs=[whole, whole, pl.BlockSpec(gain_shape, lambda i, c: (0, 0))] + [away] * 7,
            scratch_shapes=[pltpu.VMEM((rows, width), BF16), pltpu.VMEM((rows, model), F32), pltpu.VMEM((rows, model), F32),
                            pltpu.VMEM((3, 4, model // pieces, share), BF16), pltpu.VMEM((3, 2, share // pieces, model), BF16),
                            pltpu.VMEM((3,) + qk.shape[1:], BF16), pltpu.VMEM((3,) + vo.shape[1:], BF16),
                            pltpu.SemaphoreType.DMA((3, 8)), pltpu.SemaphoreType.DMA((3, 9 + model // o_size))],
        ),
        out_shape=[bf16(rows, model), bf16(rows, model), jax.ShapeDtypeStruct(gain_shape, F32)]
        + [bf16(model, 2 * share), bf16(model, 2 * share), bf16(2 * share, model)] + [bf16(*weight.shape) for weight in (w_q, w_k, w_v, w_o)],
        compiler_params=pltpu.CompilerParams(vmem_limit_bytes=56 * 2 ** 20),
        cost_estimate=pl.CostEstimate(flops=2 * pieces * rows * width * model, bytes_accessed=14 * rows * model + 2 * pieces * width * (rows + model), transcendentals=0),
    )(core, lead, rest, x, dy, mlp_out, d_norm, gain, w_q, w_k, w_v, w_o, *own_grads, *partner_grads, qk, vo)


def share_kernel(gain_ref, norm_ref, parts, send_sem, recv_sem, *, count):
    me = lax.axis_index('sp')
    rows = gain_ref.shape[0]
    meet(count)
    copies = [pltpu.make_async_remote_copy(src_ref=src, dst_ref=parts.at[me, pl.ds(j * rows, rows)], send_sem=send_sem.at[i, j], recv_sem=recv_sem.at[i, j],
                                           device_id={'sp': device}, device_id_type=MESH)
              for i, device in enumerate(other_devices(count)) for j, src in enumerate((gain_ref, norm_ref))]
    for copy in copies:
        copy.start()
    parts[pl.ds(me, 1), :rows] = gain_ref[...][None]
    parts[pl.ds(me, 1), rows:] = norm_ref[...][None]
    for copy in copies:
        copy.wait()


def settle_kernel(parts, gain_out, q_out, k_out):
    count = parts.shape[0]
    rows = gain_out.shape[0]
    heads = q_out.shape[0] // count
    gain_out[...] = jnp.sum(parts[:, :rows], axis=0)
    for device in range(count):
        q_out[device * heads:(device + 1) * heads, :] = parts[device, rows:rows + heads, :]
        k_out[device:device + 1, :] = parts[device, rows + heads:rows + heads + 1, :]


def share_small(gain, norms, q_norm, k_norm, count):
    vmem = pl.BlockSpec(memory_space=pltpu.VMEM)
    dma = pltpu.SemaphoreType.DMA((count - 1, 2))
    parts = pl.pallas_call(
        functools.partial(share_kernel, count=count),
        in_specs=[vmem] * 2,
        out_specs=vmem,
        out_shape=jax.ShapeDtypeStruct((count, 2 * gain.shape[0], gain.shape[1]), F32),
        scratch_shapes=[dma, dma],
        compiler_params=pltpu.CompilerParams(collective_id=2, has_side_effects=True),
    )(gain, norms)
    return pl.pallas_call(
        settle_kernel,
        in_specs=[vmem],
        out_specs=[vmem] * 3,
        out_shape=[jax.ShapeDtypeStruct(part.shape, F32) for part in (gain, q_norm, k_norm)],
    )(parts)


def solution(mesh):
    n_sp = mesh.shape['sp']
    seq_spec = P('dp', 'sp', None)
    grad_spec = P('dp', None)

    def layer_step(x_in, grad_y, positions, w_q, w_k, w_v, w_o, w_gate, w_up, w_down, norm_gain, q_norm, k_norm):
        batch, piece, model = x_in.shape
        num_heads, dim = q_norm.shape
        heads = num_heads // k_norm.shape[0]
        ffn = w_gate.shape[1]
        tokens = batch * piece
        me = lax.axis_index('sp')
        ahead = batch // 4
        gain_row = norm_gain.reshape(1, model)
        x_rows, dy_own = x_in.reshape(tokens, model), grad_y.reshape(tokens, model)
        n_own = input_norm(x_rows, gain_row)

        inv_freq = ROPE_THETA ** (-(jnp.arange(dim // 2, dtype=F32) * 2.0) / dim)
        angles = jnp.repeat(positions.astype(F32)[:, None] * inv_freq[None, :], 2, axis=1)
        sign = jnp.where(jnp.arange(dim) % 2 == 0, -1.0, 1.0).astype(F32)
        rope_own = jnp.stack([jnp.cos(angles), jnp.sin(angles) * sign[None, :]])

        mlp_out, d_norm, n_all, dy_all, mix, lead, norm_grads, qk, vo = front(n_own, dy_own, w_gate, w_up, w_down, rope_own, w_q, w_k, w_v, w_o, q_norm, k_norm,
                                                                        n_sp, piece, ahead, ffn // 6)
        by_tile = lambda part: part.reshape(n_sp, -1, part.shape[-1])
        *grads, rest, qk, vo = all_mlp(by_tile(n_all), by_tile(dy_all), w_gate, w_up, w_down, mix, ahead, qk, vo, ffn // 6)

        y_out, grad_x, grad_gain, full_gate, full_up, full_down, full_q, full_k, full_v, full_o = finish(
            (me % 2).reshape(1), by_tile(lead), by_tile(rest), x_rows, dy_own, mlp_out, d_norm, gain_row, w_q, w_k, w_v, w_o, grads[:3], grads[3:], qk, vo, heads * dim, dim)
        full_gain, full_qn, full_kn = share_small(grad_gain, norm_grads, q_norm, k_norm, n_sp)
        return (y_out.reshape(x_in.shape), grad_x.reshape(x_in.shape), full_q, full_k, full_v, full_o, full_gate, full_up, full_down,
                full_gain.reshape(model), full_qn, full_kn)

    in_specs = (seq_spec, seq_spec, P(('dp', 'sp'))) + (P(),) * 10
    out_specs = (seq_spec, seq_spec) + (grad_spec,) * 7 + (P('dp'), grad_spec, grad_spec)
    return jax.shard_map(layer_step, mesh=mesh, in_specs=in_specs, out_specs=out_specs, check_vma=False)
```
